32 devices in a mesh: pipe: 4 (over x, core), mp: 8 (over z, y).
Axes of the slice: x: 2, y: 2, z: 4, core: 2. Of those that a mesh axis runs over, the one named last changes fastest.
Arguments:
- hidden_in: bfloat16 [32, 8192], P(None, 'mp'), may hold values from -24000 to 24000
- lengths: int32 [32], replicated, may hold values from 1 to 256
- assign: int32 [32], replicated, may hold values from 0 to 31, each once
- token_ids: int32 [32], replicated, may hold values from 0 to 12287
- attn_gain: bfloat16 [4, 8192], P('pipe', 'mp'), may hold values from 0.099609375 to 1.8984375
- qkv_weight: bfloat16 [4, 8192, 5120], P('pipe', 'mp'), may hold values from -0.0625 to 0.0625
- qkv_bias: bfloat16 [4, 5120], P('pipe'), may hold values from -3 to 3
- out_weight: bfloat16 [4, 4096, 8192], P('pipe', None, 'mp'), may hold values from -0.375 to 0.375
- kv_cache: bfloat16 [4, 32, 2, 4, 256, 128], P('pipe', 'mp'), may hold values from -120 to 120
- final_gain: bfloat16 [8192], P('mp'), may hold values from 0.099609375 to 1.8984375
- head_weight: bfloat16 [8192, 12288], P(None, ('pipe', 'mp')), may hold values from -0.9923308 to 0.9923308
Outputs:
- logprobs: float32 [32, 12288], P(None, ('pipe', 'mp'))
- chosen: float32 [32], replicated
The draws below stay inside these ranges and needn't reach their ends.
Inputs may be any that keep to these rules, and one draw needn't show every extreme that they name: `assign`: a permutation of the 32 requests.
All inputs are finite; a program needn't handle non-finite values.
Results may differ from the reference program's by a relative error of at most 0.0017.
Values may be sent and summed in bfloat16 or wider, within the bound.
A program may use at most 64 MiB of HBM per device.

```python
import math
import jax
import jax.numpy as jnp
import numpy as np
from jax import lax

D = 8192
HEADS = 32
KV_HEADS = 4
HEAD_DIM = 128
LEN = 256
LAYERS = 4
REQ = 32
QKV = 5120
VOCAB = 12288


def draw_kv_cache(key, part):
    base_draw = jnp.clip(jax.random.normal(jax.random.fold_in(key, 11), (LAYERS, REQ, 2, KV_HEADS, LEN, HEAD_DIM), jnp.float32), -4.0, 4.0)
    return base_draw.astype(jnp.bfloat16)


def column_profile(low_end, high_end):
    fraction = jnp.arange(D).astype(jnp.float32) / max(D - 1, 1)
    return low_end * jnp.exp(fraction * jnp.log(high_end / low_end))


def profiled_base(key):
    base_draw = jnp.clip(jax.random.normal(jax.random.fold_in(key, 21), (REQ, D), jnp.float32), -6.0, 6.0)
    profile = column_profile(3.0, 30.0)
    return base_draw * profile[None, :]


def draw_hidden_in(key, part):
    base_draw = profiled_base(key)
    return base_draw.astype(jnp.bfloat16)


def draw_head_weight(key, part):
    base_draw = jnp.clip(jax.random.normal(jax.random.fold_in(key, 24), (D, VOCAB), jnp.float32), -6.0, 6.0) * (3.0 * D ** (-0.5))
    return base_draw.astype(jnp.bfloat16)


def place_ends(drawn, rng, low, largest):
    place = [jax.random.randint(jax.random.fold_in(rng, axis), (), 0, length) for axis, length in enumerate(drawn.shape)]
    longest = drawn.shape.index(max(drawn.shape))
    neighbour = place[:longest] + [(place[longest] + 1) % drawn.shape[longest]] + place[longest + 1:]
    return drawn.at[tuple(place)].set(low).at[tuple(neighbour)].set(largest)


def block_scale(key, shape, pieces, least, high):
    def one(axis_at, parts):
        heights = jax.random.uniform(jax.random.fold_in(jax.random.fold_in(key, 6), axis_at), (parts,), jnp.float32, least / len(pieces), high / len(pieces))
        return jnp.repeat(jnp.exp(heights), shape[axis_at] // parts).reshape((-1,) + (1,) * (len(shape) - axis_at - 1))

    level = one(*pieces[0])
    for cut in pieces[1:]:
        level = level * one(*cut)
    return level


def rank_table(count, lean):
    portions = [(1 << 20) // math.isqrt(standing ** lean) + 1 for standing in range(1, count + 1)]
    scale = 1 + sum(portions) // (1 << 30)
    return np.cumsum(np.array([max(1, weight // scale) for weight in portions]))


def ranked_ids(own_key, extent, count, lean):
    table = rank_table(count, lean)
    ticket = jax.random.randint(jax.random.fold_in(own_key, 1), extent, 0, int(table[count - 1]))
    rank = jnp.searchsorted(jnp.asarray(table, jnp.int32), ticket, side="right")
    return jax.random.permutation(jax.random.fold_in(own_key, 2), count)[rank].astype(jnp.int32)


def bell_draw(own_key, shape, spread, bound, pieces=(), held_as=jnp.bfloat16):
    drawn = jax.random.normal(own_key, shape, jnp.float32) * spread
    if len(pieces) > 0:
        drawn = block_scale(own_key, shape, pieces, -0.22, 0.18) * drawn
    return jnp.clip(drawn, min=-bound, max=bound).astype(held_as)


def setup_inputs(seed: int = 0) -> dict:
    keys = jax.random.split(jax.random.key(seed), 12)
    return {
        "hidden_in": draw_hidden_in(jax.random.fold_in(keys[11], 71), 0),
        "lengths": place_ends(jax.random.randint(keys[1], (REQ,), 1, LEN + 1), jax.random.fold_in(keys[1], 1), 1, LEN).astype(jnp.int32),
        "assign": jax.random.permutation(keys[2], REQ).astype(jnp.int32),
        "token_ids": place_ends(ranked_ids(keys[3], (REQ,), VOCAB, 2), jax.random.fold_in(keys[3], 3), 0, VOCAB - 1).astype(jnp.int32),
        "attn_gain": jnp.clip(1.0 + 0.18 * jax.random.normal(keys[4], (LAYERS, D), jnp.float32), 0.099609375, 1.8984375).astype(jnp.bfloat16),
        "qkv_weight": bell_draw(keys[5], (LAYERS, D, QKV), D ** -0.5, 0.0625, ((0, 4), (1, 8))),
        "qkv_bias": bell_draw(keys[6], (LAYERS, QKV), 0.5, 3.0, ((0, 4),)),
        "out_weight": bell_draw(keys[7], (LAYERS, HEADS * HEAD_DIM, D), (HEADS * HEAD_DIM // 16) ** -0.5, 0.375, ((0, 4), (2, 8))),
        "kv_cache": draw_kv_cache(jax.random.fold_in(keys[11], 71), 0),
        "final_gain": jnp.clip(1.0 + 0.18 * jax.random.normal(keys[9], (D,), jnp.float32), 0.099609375, 1.8984375).astype(jnp.bfloat16),
        "head_weight": draw_head_weight(jax.random.fold_in(keys[11], 71), 0),
    }


EPS = 1e-06
THETA = 1000000.0

def rounded(values_in):
    return lax.optimization_barrier(values_in.astype(jnp.bfloat16)).astype(jnp.float32)

def rotate(values_in, positions):
    half_dim = values_in.shape[-1] // 2
    frequency = THETA ** (-jnp.arange(half_dim).astype(jnp.float32) * 2.0 / values_in.shape[-1])
    angles = positions.astype(jnp.float32)[:, None, None] * frequency[None, None, :]
    front_half = values_in[..., :half_dim]
    back_half = values_in[..., half_dim:]
    cosine = jnp.cos(angles)
    sine_part = jnp.sin(angles)
    return jnp.concatenate([front_half * cosine - back_half * sine_part, back_half * cosine + front_half * sine_part], axis=-1)

def reference(hidden_in, lengths, assign, token_ids, attn_gain, qkv_weight, qkv_bias, out_weight, kv_cache, final_gain, head_weight):
    stream = hidden_in[assign]
    positions = lengths[assign]
    group_size = HEADS // KV_HEADS
    query_cols = HEADS * HEAD_DIM
    key_cols = KV_HEADS * HEAD_DIM
    row_count = stream.shape[0]
    scale_factor = HEAD_DIM ** (-0.5)
    visible = jnp.arange(LEN).astype(jnp.int32)[None, :] < positions[:, None]
    key_mask = visible[:, None, None, :]
    for layer_index in range(LAYERS):
        current = stream.astype(jnp.float32)
        mean_sq = lax.optimization_barrier(jnp.mean(current * current, axis=1))
        scaled = (current * attn_gain[layer_index].astype(jnp.float32)).astype(jnp.bfloat16)
        projected = jnp.dot(scaled, qkv_weight[layer_index], preferred_element_type=jnp.float32)
        projected = projected * lax.rsqrt(mean_sq + EPS)[:, None] + qkv_bias[layer_index].astype(jnp.float32)
        queries = rotate(projected[:, :query_cols].reshape(row_count, HEADS, HEAD_DIM), positions).astype(jnp.bfloat16)
        key_new = rotate(projected[:, query_cols:query_cols + key_cols].reshape(row_count, KV_HEADS, HEAD_DIM), positions).astype(jnp.bfloat16)
        value_new = projected[:, query_cols + key_cols:].reshape(row_count, KV_HEADS, HEAD_DIM).astype(jnp.bfloat16)
        cache_rows = kv_cache[layer_index][assign].astype(jnp.float32)
        query_f = queries.astype(jnp.float32).reshape(row_count, KV_HEADS, group_size, HEAD_DIM)
        scores = jnp.einsum('rkgd,rkjd->rkgj', query_f, cache_rows[:, 0]) * scale_factor
        self_score = jnp.einsum('rkgd,rkd->rkg', query_f, key_new.astype(jnp.float32)) * scale_factor
        row_top = jnp.maximum(lax.optimization_barrier(jnp.max(jnp.where(key_mask, scores, -1e+30), axis=-1)), self_score)
        weights = jnp.where(key_mask, jnp.exp(scores - row_top[..., None]), 0.0)
        self_weight = jnp.exp(self_score - row_top)
        row_total = lax.optimization_barrier(jnp.sum(weights, axis=-1)) + self_weight
        summed = jnp.einsum('rkgj,rkjd->rkgd', rounded(weights), cache_rows[:, 1])
        summed = summed + rounded(self_weight)[..., None] * value_new.astype(jnp.float32)[:, :, None, :]
        attended = (summed / row_total[..., None]).astype(jnp.bfloat16).reshape(row_count, query_cols)
        update = jnp.dot(attended, out_weight[layer_index], preferred_element_type=jnp.float32)
        stream = (current + update).astype(jnp.bfloat16)
    current = stream.astype(jnp.float32)
    mean_sq = lax.optimization_barrier(jnp.mean(current * current, axis=1))
    normed = (current * final_gain.astype(jnp.float32) * lax.rsqrt(mean_sq + EPS)[:, None]).astype(jnp.bfloat16)
    logits = jnp.dot(normed, head_weight, preferred_element_type=jnp.float32)
    row_top = lax.optimization_barrier(jnp.max(logits, axis=1))
    row_total = lax.optimization_barrier(jnp.sum(jnp.exp(logits - row_top[:, None]), axis=1))
    logprobs = logits - (row_top + jnp.log(row_total))[:, None]
    targets = token_ids[assign]
    chosen = jnp.take_along_axis(logprobs, targets[:, None], axis=1)[:, 0]
    return (logprobs, chosen)
```

```python
import functools

import jax
import jax.numpy as jnp
import numpy as np
from jax import lax
from jax.experimental import pallas as pl
from jax.experimental.pallas import tpu as pltpu
from jax.sharding import PartitionSpec as P

HEADS = 32
KV_HEADS = 4
HEAD_DIM = 128
EPS = 1e-06
THETA = 1000000.0
MESH = pl.DeviceIdType.MESH
F32 = jnp.float32
BF16 = jnp.bfloat16


def remote(src, dst, send_sem, recv_sem, device):
    return pltpu.make_async_remote_copy(
        src_ref=src,
        dst_ref=dst,
        send_sem=send_sem,
        recv_sem=recv_sem,
        device_id=device,
        device_id_type=MESH,
    )


def kernel(
    sections,
    n,
    hidden,
    lengths,
    assign,
    token_ids,
    gain,
    qkv_weight,
    bias,
    out_weight,
    cache,
    final_gain,
    head_weight,
    freq,
    out,
    chosen,
    wq,
    wo,
    kv,
    hw,
    x,
    xo,
    scaled,
    stage,
    part,
    part_in,
    sq,
    sq_in,
    gain_v,
    bias_v,
    final_v,
    len_v,
    slot_v,
    token_v,
    freq_v,
    slot_s,
    bias_rows,
    turn_cos,
    turn_sin,
    own_rows,
    target_v,
    fresh,
    att,
    att_in,
    update,
    fin,
    fsq_in,
    red,
    red_in,
    flat,
    wq_sem,
    w_sem,
    small_sem,
    part_s,
    part_r,
    sq_s,
    sq_r,
    att_s,
    att_r,
    hop_s,
    hop_r,
    fin_s,
    fin_r,
    sib_s,
    sib_r,
    fsq_s,
    fsq_r,
    fp_s,
    fq_s,
    fp_r,
    red_s,
    red_r,
):
    sec = lax.axis_index("pipe")
    me = lax.axis_index("mp")
    total = sections * n
    rows, width = x.shape
    lc = kv.shape[0]
    heads_all = HEADS + 2 * KV_HEADS
    group = HEADS // KV_HEADS
    phases = heads_all // group
    span = lc * group
    last = sections - 1
    scale = HEAD_DIM ** (-0.5)
    cw = group * HEAD_DIM
    half = rows // 2
    chunks = fin.shape[2]
    chunk = width // chunks
    core = lax.rem(sec, 2)
    sibling = sec + 1 - 2 * core
    mine = sec * n + me
    early = min(2, phases)

    def mate(own, k, count):
        if count & (count - 1):
            return lax.rem(own + k, count), lax.rem(own + count - k, count)
        other = 0
        for b in range(count.bit_length() - 1):
            place = 1 << b
            mine_bit = lax.rem(own // place, 2)
            if isinstance(k, int):
                bit = 1 - mine_bit if (k // place) % 2 else mine_bit
            else:
                flip = lax.rem(k // place, 2)
                bit = mine_bit + flip - 2 * mine_bit * flip
            other = other + place * bit
        return other, other

    pairs = [mate(me, k, n) for k in range(n)]
    far_first = range(n - 1, 0, -1)

    def to_peer(k):
        return pairs[k][0]

    def from_peer(k):
        return pairs[k][1]

    def wq_copy(c):
        cols = pl.ds(pl.multiple_of(c * cw, cw), cw)
        return pltpu.make_async_copy(qkv_weight.at[0, :, cols], wq.at[:, cols], wq_sem.at[c])

    def phase_of(k):
        return lax.rem(k + phases - 1, phases)

    def small(i, src, dst):
        return pltpu.make_async_copy(src, dst, small_sem.at[i])

    hidden_copy = small(0, hidden, x)
    gain_copy = small(1, gain, gain_v)
    others = [
        small(2, bias, bias_v),
        small(3, final_gain, final_v),
        small(4, lengths, len_v),
        small(5, assign, slot_v),
        small(6, token_ids, token_v),
        small(7, freq, freq_v),
        small(8, assign, slot_s),
    ]

    @pl.when(sec == 0)
    def _():
        hidden_copy.start()

    gain_copy.start()
    for k in range(early):
        wq_copy((k + phases - 1) % phases).start()

    def wq_rest():
        for k in range(early, phases):
            wq_copy((k + phases - 1) % phases).start()

    kv_copy = pltpu.make_async_copy(cache.at[0], kv, w_sem.at[0])
    wo_copy = pltpu.make_async_copy(out_weight.at[0], wo, w_sem.at[1])
    hw_copy = pltpu.make_async_copy(head_weight, hw, w_sem.at[2])

    barrier = pltpu.get_barrier_semaphore()
    for k in far_first:
        pl.semaphore_signal(barrier, inc=1, device_id=(sec, to_peer(k)), device_id_type=MESH)
    for k in range(1, sections):
        pl.semaphore_signal(
            barrier, inc=1, device_id=(lax.rem(sec + k, sections), me), device_id_type=MESH
        )
    @pl.when(sec > 0)
    def _():
        for copy in others:
            copy.start()
        wq_rest()
        kv_copy.start()
        wo_copy.start()
        hw_copy.start()

    eye = lax.broadcasted_iota(jnp.int32, (rows, 128), 0) == lax.broadcasted_iota(
        jnp.int32, (rows, 128), 1
    )

    def to_row(col):
        return jnp.sum(jnp.where(eye, col, 0.0), axis=0, keepdims=True)

    def to_col(row):
        return jnp.sum(jnp.where(eye, row, 0.0), axis=1, keepdims=True)

    lane = lax.broadcasted_iota(jnp.int32, (1, HEAD_DIM), 1)
    lane_rows = lax.broadcasted_iota(jnp.int32, (1, rows), 1)
    small_eye = lax.broadcasted_iota(jnp.int32, (rows, rows), 0) == lax.broadcasted_iota(
        jnp.int32, (rows, rows), 1
    )

    def set_up():
        for copy in others:
            copy.wait()
        for i in range(heads_all):
            bias_rows[i : i + 1, :] = bias_v[:, i * HEAD_DIM : (i + 1) * HEAD_DIM].astype(F32)
        target = jnp.sum(
            jnp.where(small_eye, token_v[...].astype(F32), 0.0), axis=1, keepdims=True
        )
        target_v[...] = jnp.broadcast_to(target, target_v.shape)
        for i in range(lc):
            length = jnp.sum(
                jnp.where(lane_rows == me * lc + i, len_v[...].astype(F32), 0.0),
                axis=1,
                keepdims=True,
            )
            own_rows[i : i + 1, :] = jnp.broadcast_to(length, (1, HEAD_DIM))
        angles = own_rows[...] * freq_v[...]
        turn_cos[...] = jnp.cos(angles)
        turn_sin[...] = jnp.sin(angles) * jnp.where(lane < HEAD_DIM // 2, -1.0, 1.0)

    def scale_rows():
        gain_copy.wait()
        current = x[...].astype(F32)
        sq[...] = jnp.broadcast_to(
            to_row(jnp.sum(current * current, axis=1, keepdims=True)), sq.shape
        )
        scaled[...] = (current * gain_v[...].astype(F32)).astype(BF16)

    def sq_copy(peer, slot):
        return remote(sq, sq_in.at[slot], sq_s, sq_r, (sec, peer))

    def sq_send():
        for k in far_first:
            sq_copy(to_peer(k), me).start()
        sq_in[me] = sq[...]

    def part_copy(phase, peer, slot):
        return remote(
            part.at[phase, peer],
            part_in.at[phase, slot],
            part_s,
            part_r.at[phase],
            (sec, peer),
        )

    def multiply(phase):
        wq_copy(phase).wait()
        base = pl.multiple_of(phase * cw, cw)
        piece = jnp.dot(scaled[...], wq[:, pl.ds(base, cw)], preferred_element_type=F32)
        for j in range(group):
            stage[pl.ds(j, rows, stride=group), :] = piece[
                :, j * HEAD_DIM : (j + 1) * HEAD_DIM
            ]
        for p in range(n):
            part[phase, p] = stage[p * span : (p + 1) * span, :].astype(BF16)

    def spread(phase):
        for k in far_first:
            part_copy(phase, to_peer(k), me).start()
        part_in[phase, me] = part[phase, me]

    def compute_only(k, carry):
        multiply(phase_of(k))
        return carry

    def send_only(k, carry):
        spread(phase_of(k))
        return carry

    def project(k, carry):
        multiply(phase_of(k))
        spread(phase_of(k))
        return carry

    def hop_copy(c, to):
        cols = pl.ds(c * chunk, chunk)
        return remote(xo.at[:, cols], x.at[:, cols], hop_s, hop_r, (to, me))


    @pl.when(sec == 0)
    def _():
        hidden_copy.wait()
        scale_rows()
        wq_rest()
        for copy in others:
            copy.start()
        lax.fori_loop(0, early, compute_only, 0)

    @pl.when(sec > 0)
    def _():
        set_up()

    pl.semaphore_wait(barrier, n + sections - 2)

    @pl.when(sec == 0)
    def _():
        sq_send()
        lax.fori_loop(0, early, send_only, 0)

    @pl.when(sec > 0)
    def _():
        remote(xo, x, hop_s, hop_r, (sec - 1, me)).wait_recv()
        scale_rows()
        sq_send()

    lax.fori_loop(jnp.where(sec == 0, early, 0), phases, project, 0)

    @pl.when(sec == 0)
    def _():
        kv_copy.start()
        wo_copy.start()
        hw_copy.start()
        set_up()

    def summed(phase):
        remote(
            part.at[phase, pl.ds(1, n - 1)],
            part_in.at[phase, pl.ds(1, n - 1)],
            part_s,
            part_r.at[phase],
            (sec, me),
        ).wait_recv()
        result = part_in[phase, 0].astype(F32)
        for p in range(1, n):
            result = result + part_in[phase, p].astype(F32)
        return result

    remote(
        sq_in.at[pl.ds(1, n - 1)], sq_in.at[pl.ds(1, n - 1)], sq_s, sq_r, (sec, me)
    ).wait_recv()
    squares = sq_in[0]
    for p in range(1, n):
        squares = squares + sq_in[p]
    factor = [
        lax.rsqrt(
            jnp.sum(
                jnp.where(lane == me * lc + i, squares[0:1, :], 0.0), axis=1, keepdims=True
            )
            / (n * width)
            + EPS
        )
        for i in range(lc)
    ]
    own_len = [own_rows[i : i + 1, 0:1] for i in range(lc)]
    cosine = turn_cos[...]
    sine = turn_sin[...]

    def turn(block, i):
        return (
            block * cosine[i : i + 1]
            + pltpu.roll(block, HEAD_DIM // 2, 1) * sine[i : i + 1]
        )

    is_key = lax.broadcasted_iota(jnp.int32, (2 * KV_HEADS, HEAD_DIM), 0) < KV_HEADS
    block_sum = summed(phases - 1)
    for i in range(lc):
        block = block_sum[i * group : (i + 1) * group] * factor[i] + bias_rows[HEADS:, :]
        fresh[i] = jnp.where(is_key, turn(block, i), block).astype(BF16).astype(F32)
    kv_copy.wait()
    pos = lax.broadcasted_iota(jnp.int32, (1, kv.shape[3]), 1).astype(F32)

    def att_copy(h, peer, slot):
        return remote(
            att.at[h], att_in.at[h, slot], att_s, att_r.at[h], (sec, peer)
        )

    def attend(h, carry):
        block_sum = summed(h)
        bias_h = bias_rows[pl.ds(pl.multiple_of(h * group, group), group), :]
        done = []
        for i in range(lc):
            block = block_sum[i * group : (i + 1) * group] * factor[i] + bias_h
            query = turn(block, i).astype(BF16)
            key_new = fresh[i, pl.ds(h, 1), :]
            value_new = fresh[i, pl.ds(KV_HEADS + h, 1), :]
            visible = pos < own_len[i]
            scores = (
                lax.dot_general(
                    query,
                    kv[i, 0, h],
                    (((1,), (1,)), ((), ())),
                    preferred_element_type=F32,
                )
                * scale
            )
            self_score = (
                jnp.sum(query.astype(F32) * key_new, axis=1, keepdims=True) * scale
            )
            top = jnp.maximum(
                jnp.max(jnp.where(visible, scores, -1e30), axis=1, keepdims=True), self_score
            )
            weights = jnp.where(visible, jnp.exp(scores - top), 0.0)
            self_weight = jnp.exp(self_score - top)
            denominator = jnp.sum(weights, axis=1, keepdims=True) + self_weight
            mixed = jnp.dot(weights.astype(BF16), kv[i, 1, h], preferred_element_type=F32)
            mixed = mixed + self_weight.astype(BF16).astype(F32) * value_new
            done.append(mixed / denominator)
        att[h] = jnp.concatenate(done, axis=0).astype(BF16)
        for k in far_first:
            att_copy(h, to_peer(k), me).start()
        att_in[h, me] = att[h]
        return carry

    lax.fori_loop(0, KV_HEADS, attend, 0)
    wo_copy.wait()
    update[...] = x[...].astype(F32)

    def all_att(h):
        return remote(
            att_in.at[h, pl.ds(1, n - 1)],
            att_in.at[h, pl.ds(1, n - 1)],
            att_s,
            att_r.at[h],
            (sec, me),
        )

    def gathered(h):
        all_att(h).wait_recv()
        for p in range(n):
            stage[p * span : (p + 1) * span, :] = att_in[h, p].astype(F32)
        return jnp.concatenate(
            [stage[pl.ds(j, rows, stride=group), :].astype(BF16) for j in range(group)],
            axis=1,
        )

    def project_out(h, carry):
        mat = gathered(h)
        depth = pl.ds(pl.multiple_of(h * cw, cw), cw)
        update[...] += jnp.dot(mat, wo[depth, :], preferred_element_type=F32)
        return carry

    lax.fori_loop(0, KV_HEADS - 1, project_out, 0)

    def fin_copy(c, peer, slot):
        return remote(
            fin.at[core, slot, c],
            fin.at[core, slot, c],
            fin_s,
            fin_r.at[slot],
            (sec, peer),
        )

    def sib_copy(c, piece, slot):
        return remote(
            fin.at[piece, slot, c],
            fin.at[piece, slot, c],
            sib_s,
            sib_r.at[slot],
            (sibling, me),
        )

    def fsq_copy(peer, slot):
        return remote(
            fsq_in.at[slot], fsq_in.at[slot], fsq_s, fsq_r, (sec, peer)
        )

    def fp_copy(c, k):
        to = lax.rem(sec + k, sections)
        piece = lax.rem(to, 2)
        return remote(
            fin.at[piece, me, c], fin.at[piece, me, c], fp_s, fp_r.at[c], (to, me)
        )

    def fp_sq(k):
        to = lax.rem(sec + k, sections)
        return remote(
            fsq_in.at[me], fsq_in.at[me], fq_s, fp_r.at[chunks], (to, me)
        )

    mat = gathered(KV_HEADS - 1)
    top_rows = (KV_HEADS - 1) * cw
    final_sq = jnp.zeros((rows, 1), F32)
    for c in range(chunks):
        cols = slice(c * chunk, (c + 1) * chunk)
        grown = update[:, cols] + jnp.dot(
            mat, wo[top_rows : top_rows + cw, cols], preferred_element_type=F32
        )
        new = grown.astype(BF16)
        xo[:, cols] = new
        final = new.astype(F32)
        final_sq = final_sq + jnp.sum(final * final, axis=1, keepdims=True)

        @pl.when(sec < last)
        def _():
            hop_copy(c, sec + 1).start()

        @pl.when(sec == last)
        def _():
            lanes = chunk // 128
            row = jnp.concatenate(
                [final_v[c * lanes + i : c * lanes + i + 1, :].astype(F32) for i in range(lanes)],
                axis=1,
            )
            both = (final * row).astype(BF16)
            fin[0, me, c] = both[:half]
            fin[1, me, c] = both[half:]
            for k in range(1, sections):
                fp_copy(c, k).start()
            for k in far_first:
                fin_copy(c, to_peer(k), me).start()
            sib_copy(c, core, me).start()

    @pl.when(sec == last)
    def _():
        fsq_in[me] = to_row(final_sq)
        for k in range(1, sections):
            fp_sq(k).start()
        for k in far_first:
            fsq_copy(to_peer(k), me).start()

    @pl.when(sec < last)
    def _():
        for c in range(chunks):
            arriving = remote(
                fin.at[core, me, c], fin.at[core, me, c], fp_s, fp_r.at[c], (last, me)
            )
            arriving.wait_recv()
            for k in far_first:
                fin_copy(c, to_peer(k), me).start()

            @pl.when(sec < last - 1)
            def _():
                sib_copy(c, core, me).start()

        arriving = remote(
            fsq_in.at[me], fsq_in.at[me], fq_s, fp_r.at[chunks], (last, me)
        )
        arriving.wait_recv()
        for k in far_first:
            fsq_copy(to_peer(k), me).start()

    hw_copy.wait()

    def whole(piece, slot, send, recv):
        return remote(fin.at[piece, slot], fin.at[piece, slot], send, recv.at[slot], (sibling, me))

    def pass_on(k):
        _, peer = mate(me, k, n)
        whole(core, peer, fin_s, fin_r).wait_recv()
        for c in range(chunks):
            sib_copy(c, core, peer).start()

    def head(k, logits):
        _, peer = mate(me, k, n)
        if isinstance(k, int) and k == 0:

            @pl.when(sec < last)
            def _():
                whole(1 - core, peer, sib_s, sib_r).wait_recv()

        else:
            whole(1 - core, peer, sib_s, sib_r).wait_recv()
        for c in range(chunks):
            at = pl.ds(pl.multiple_of(peer * width + c * chunk, chunk), chunk)
            both = jnp.concatenate([fin[0, peer, c], fin[1, peer, c]], axis=0)
            logits = logits + jnp.dot(both, hw[at, :], preferred_element_type=F32)
        return logits

    lag = min(2, n - 1)
    for k in range(1, lag + 1):
        pass_on(k)
    logits = head(0, jnp.zeros(out.shape, F32))

    def step(k, logits):
        pass_on(k)
        return head(k - lag, logits)

    logits = lax.fori_loop(lag + 1, n, step, logits)
    logits = lax.fori_loop(n - lag, n, head, logits)
    all_fsq = remote(
        fsq_in.at[pl.ds(1, n - 1)], fsq_in.at[pl.ds(1, n - 1)], fsq_s, fsq_r, (sec, me)
    )
    all_fsq.wait_recv()
    squares = jnp.sum(fsq_in[:, 0, :], axis=0, keepdims=True)
    logits = logits * lax.rsqrt(to_col(squares) / (n * width) + EPS)
    vocab = out.shape[1]
    ids = (mine * vocab + lax.broadcasted_iota(jnp.int32, (1, vocab), 1)).astype(F32)
    picked = jnp.sum(jnp.where(ids == target_v[:, 0:1], logits, 0.0), axis=1, keepdims=True)
    top = jnp.max(logits, axis=1, keepdims=True)
    amount = jnp.sum(jnp.exp(logits - top), axis=1, keepdims=True)
    row_of = lax.broadcasted_iota(jnp.int32, (rows, 128), 0)
    lane_of = lax.broadcasted_iota(jnp.int32, (rows, 128), 1)
    packed = jnp.where(lane_of == row_of, top, 0.0)
    packed = jnp.where(lane_of == row_of + rows, amount, packed)
    packed = jnp.where(lane_of == row_of + 2 * rows, picked, packed)
    red[...] = jnp.sum(packed, axis=0, keepdims=True)

    def red_copy(other, slot):
        return remote(
            red, red_in.at[slot], red_s, red_r, (other // n, lax.rem(other, n))
        )

    if total <= 64:
        for k in range(total - 1, 0, -1):
            red_copy(mate(mine, k, total)[0], mine).start()
    else:

        def red_start(k, carry):
            red_copy(mate(mine, total - k, total)[0], mine).start()
            return carry

        lax.fori_loop(1, total, red_start, 0)
    red_in[mine] = red[...]
    flat[...] = logits

    def sent(ref, sem):
        remote(ref, ref, sem, sem, (sec, me)).wait_send()

    others_n = pl.ds(1, n - 1)
    sent(sq_in.at[others_n], sq_s)
    sent(part_in.at[:, others_n], part_s)
    sent(att_in.at[:, others_n], att_s)
    sent(fin.at[0, others_n], fin_s)
    sent(fin.at[0, others_n], sib_s)
    all_fsq.wait_send()

    @pl.when(sec != last - 1)
    def _():
        sent(fin.at[0, 0], sib_s)

    @pl.when(sec < last)
    def _():
        sent(xo, hop_s)

    @pl.when(sec == last)
    def _():
        sent(fin.at[0, pl.ds(1, sections - 1)], fp_s)
        sent(fsq_in.at[pl.ds(1, sections - 1)], fq_s)

    order = (
        jnp.sum(jnp.where(small_eye, slot_v[...].astype(F32), 0.0), axis=1, keepdims=True)
        == lane_of.astype(F32)
    )
    for s in range(rows):
        out[s : s + 1, :] = flat[pl.ds(slot_s[0, s], 1), :]

    everyone = remote(
        red_in.at[pl.ds(1, total - 1)],
        red_in.at[pl.ds(1, total - 1)],
        red_s,
        red_r,
        (sec, me),
    )
    everyone.wait_recv()
    seen = red_in[:, 0, :]
    row_top = jnp.max(seen, axis=0, keepdims=True)
    amounts = pltpu.roll(seen, 128 - rows, 1)
    row_total = jnp.sum(amounts * jnp.exp(jnp.minimum(seen - row_top, 0.0)), axis=0, keepdims=True)
    log_total = row_top + jnp.log(row_total)
    total_col = jnp.sum(jnp.where(order, log_total, 0.0), axis=1, keepdims=True)
    out[...] = out[...] - total_col
    scored = pltpu.roll(jnp.sum(seen, axis=0, keepdims=True), 128 - 2 * rows, 1) - log_total
    chosen[...] = to_row(jnp.sum(jnp.where(order, scored, 0.0), axis=1, keepdims=True))
    everyone.wait_send()


def local(
    hidden_in,
    lengths,
    assign,
    token_ids,
    attn_gain,
    qkv_weight,
    qkv_bias,
    out_weight,
    kv_cache,
    final_gain,
    head_weight,
):
    sections = lax.axis_size("pipe")
    n = lax.axis_size("mp")
    rows, width = hidden_in.shape
    lc = kv_cache.shape[1]
    qkv = qkv_weight.shape[2]
    inner = out_weight.shape[1]
    vocab = head_weight.shape[1]
    heads_all = HEADS + 2 * KV_HEADS
    half = HEAD_DIM // 2
    frequency = np.float32(THETA) ** (
        -np.arange(half).astype(np.float32) * np.float32(2.0) / np.float32(HEAD_DIM)
    )
    freq = jnp.asarray(np.concatenate([frequency, frequency])[None, :], F32)
    group = HEADS // KV_HEADS
    phases = heads_all // group
    span = lc * group
    dma = pltpu.SemaphoreType.DMA
    vm = pl.BlockSpec(memory_space=pltpu.VMEM)
    hbm = pl.BlockSpec(memory_space=pltpu.HBM)
    total = sections * n
    chunks = 2
    logprobs, chosen = pl.pallas_call(
        functools.partial(kernel, sections, n),
        out_shape=(
            jax.ShapeDtypeStruct((rows, vocab), F32),
            jax.ShapeDtypeStruct((1, 128), F32),
        ),
        in_specs=[hbm] * 12,
        out_specs=(vm, vm),
        scratch_shapes=[
            pltpu.VMEM((width, qkv), BF16),
            pltpu.VMEM((inner, width), BF16),
            pltpu.VMEM(kv_cache.shape[1:], BF16),
            pltpu.VMEM(head_weight.shape, BF16),
            pltpu.VMEM((rows, width), BF16),
            pltpu.VMEM((rows, width), BF16),
            pltpu.VMEM((rows, width), BF16),
            pltpu.VMEM((rows * group, HEAD_DIM), F32),
            pltpu.VMEM((phases, n, span, HEAD_DIM), BF16),
            pltpu.VMEM((phases, n, span, HEAD_DIM), BF16),
            pltpu.VMEM((8, 128), F32),
            pltpu.VMEM((n, 8, 128), F32),
            pltpu.VMEM((1, width), BF16),
            pltpu.VMEM((1, qkv), BF16),
            pltpu.VMEM((width // 128, 128), BF16),
            pltpu.VMEM((1, rows), jnp.int32),
            pltpu.VMEM((1, rows), jnp.int32),
            pltpu.VMEM((1, rows), jnp.int32),
            pltpu.VMEM((1, HEAD_DIM), F32),
            pltpu.SMEM((1, rows), jnp.int32),
            pltpu.VMEM((heads_all, HEAD_DIM), F32),
            pltpu.VMEM((lc, HEAD_DIM), F32),
            pltpu.VMEM((lc, HEAD_DIM), F32),
            pltpu.VMEM((lc, HEAD_DIM), F32),
            pltpu.VMEM((rows, 128), F32),
            pltpu.VMEM((lc, 2 * KV_HEADS, HEAD_DIM), F32),
            pltpu.VMEM((KV_HEADS, span, HEAD_DIM), BF16),
            pltpu.VMEM((KV_HEADS, n, span, HEAD_DIM), BF16),
            pltpu.VMEM((rows, width), F32),
            pltpu.VMEM((2, n, chunks, rows // 2, width // chunks), BF16),
            pltpu.VMEM((n, 1, 128), F32),
            pltpu.VMEM((1, 128), F32),
            pltpu.VMEM((total, 1, 128), F32),
            pltpu.VMEM((rows, vocab), F32),
            dma((phases,)),
            dma((3,)),
            dma((9,)),
            dma,
            dma((phases,)),
            dma,
            dma,
            dma,
            dma((KV_HEADS,)),
            dma,
            dma,
            dma,
            dma((n,)),
            dma,
            dma((n,)),
            dma,
            dma,
            dma,
            dma,
            dma((chunks + 1,)),
            dma,
            dma,
        ],
        compiler_params=pltpu.CompilerParams(
            collective_id=0, has_side_effects=True, vmem_limit_bytes=60 * 1024 * 1024
        ),
    )(
        hidden_in,
        lengths.reshape(1, rows),
        assign.reshape(1, rows),
        token_ids.reshape(1, rows),
        attn_gain,
        qkv_weight,
        qkv_bias,
        out_weight,
        kv_cache,
        final_gain.reshape(width // 128, 128),
        head_weight,
        freq,
    )
    return logprobs, chosen[0, :rows]


def solution(mesh):
    return jax.shard_map(
        local,
        mesh=mesh,
        in_specs=(
            P(None, "mp"),
            P(),
            P(),
            P(),
            P("pipe", "mp"),
            P("pipe", "mp", None),
            P("pipe", None),
            P("pipe", None, "mp"),
            P("pipe", "mp", None, None, None, None),
            P("mp"),
            P(None, ("pipe", "mp")),
        ),
        out_specs=(P(None, ("pipe", "mp")), P()),
        check_vma=False,
    )
```

```python
import functools

import jax
import jax.numpy as jnp
import numpy as np
from jax import lax
from jax.experimental import pallas as pl
from jax.experimental.pallas import tpu as pltpu
from jax.sharding import PartitionSpec as P

HEADS = 32
KV_HEADS = 4
HEAD_DIM = 128
EPS = 1e-06
THETA = 1000000.0
MESH = pl.DeviceIdType.MESH
F32 = jnp.float32
BF16 = jnp.bfloat16


def remote(src, dst, send_sem, recv_sem, device):
    return pltpu.make_async_remote_copy(
        src_ref=src,
        dst_ref=dst,
        send_sem=send_sem,
        recv_sem=recv_sem,
        device_id=device,
        device_id_type=MESH,
    )


def kernel(
    sections,
    n,
    hidden,
    lengths,
    assign,
    token_ids,
    gain,
    qkv_weight,
    bias,
    out_weight,
    cache,
    final_gain,
    head_weight,
    freq,
    out,
    chosen,
    wq,
    wo,
    kv,
    hw,
    x,
    xo,
    scaled,
    stage,
    part,
    part_in,
    sq,
    sq_in,
    gain_v,
    bias_v,
    final_v,
    len_v,
    slot_v,
    token_v,
    freq_v,
    slot_s,
    bias_rows,
    turn_cos,
    turn_sin,
    own_rows,
    target_v,
    fresh,
    att,
    att_in,
    update,
    fin,
    fsq_in,
    red,
    red_in,
    flat,
    wq_sem,
    w_sem,
    small_sem,
    part_s,
    part_r,
    sq_s,
    sq_r,
    att_s,
    att_r,
    hop_s,
    hop_r,
    fin_s,
    fin_r,
    sib_s,
    sib_r,
    fsq_s,
    fsq_r,
    fp_s,
    fq_s,
    fp_r,
    red_s,
    red_r,
):
    sec = lax.axis_index("pipe")
    me = lax.axis_index("mp")
    total = sections * n
    rows, width = x.shape
    lc = kv.shape[0]
    heads_all = HEADS + 2 * KV_HEADS
    group = HEADS // KV_HEADS
    phases = heads_all // group
    span = lc * group
    last = sections - 1
    scale = HEAD_DIM ** (-0.5)
    cw = group * HEAD_DIM
    half = rows // 2
    chunks = fin.shape[2]
    chunk = width // chunks
    core = lax.rem(sec, 2)
    sibling = sec + 1 - 2 * core
    mine = sec * n + me
    early = min(2, phases)

    def mate(own, k, count):
        if count & (count - 1):
            return lax.rem(own + k, count), lax.rem(own + count - k, count)
        other = 0
        for b in range(count.bit_length() - 1):
            place = 1 << b
            mine_bit = lax.rem(own // place, 2)
            if isinstance(k, int):
                bit = 1 - mine_bit if (k // place) % 2 else mine_bit
            else:
                flip = lax.rem(k // place, 2)
                bit = mine_bit + flip - 2 * mine_bit * flip
            other = other + place * bit
        return other, other

    pairs = [mate(me, k, n) for k in range(n)]
    far_first = range(n - 1, 0, -1)

    def to_peer(k):
        return pairs[k][0]

    def from_peer(k):
        return pairs[k][1]

    def wq_copy(c):
        cols = pl.ds(pl.multiple_of(c * cw, cw), cw)
        return pltpu.make_async_copy(qkv_weight.at[0, :, cols], wq.at[:, cols], wq_sem.at[c])

    def phase_of(k):
        return lax.rem(k + phases - 1, phases)

    def small(i, src, dst):
        return pltpu.make_async_copy(src, dst, small_sem.at[i])

    hidden_copy = small(0, hidden, x)
    gain_copy = small(1, gain, gain_v)
    others = [
        small(2, bias, bias_v),
        small(3, final_gain, final_v),
        small(4, lengths, len_v),
        small(5, assign, slot_v),
        small(6, token_ids, token_v),
        small(7, freq, freq_v),
        small(8, assign, slot_s),
    ]

    @pl.when(sec == 0)
    def _():
        hidden_copy.start()

    gain_copy.start()
    for k in range(early):
        wq_copy((k + phases - 1) % phases).start()

    def wq_rest():
        for k in range(early, phases):
            wq_copy((k + phases - 1) % phases).start()

    kv_copy = pltpu.make_async_copy(cache.at[0], kv, w_sem.at[0])
    wo_copy = pltpu.make_async_copy(out_weight.at[0], wo, w_sem.at[1])
    hw_copy = pltpu.make_async_copy(head_weight, hw, w_sem.at[2])

    barrier = pltpu.get_barrier_semaphore()
    for k in far_first:
        pl.semaphore_signal(barrier, inc=1, device_id=(sec, to_peer(k)), device_id_type=MESH)
    for k in range(1, sections):
        pl.semaphore_signal(
            barrier, inc=1, device_id=(lax.rem(sec + k, sections), me), device_id_type=MESH
        )
    @pl.when(sec > 0)
    def _():
        for copy in others:
            copy.start()
        wq_rest()
        kv_copy.start()
        wo_copy.start()
        hw_copy.start()

    eye = lax.broadcasted_iota(jnp.int32, (rows, 128), 0) == lax.broadcasted_iota(
        jnp.int32, (rows, 128), 1
    )

    def to_row(col):
        return jnp.sum(jnp.where(eye, col, 0.0), axis=0, keepdims=True)

    def to_col(row):
        return jnp.sum(jnp.where(eye, row, 0.0), axis=1, keepdims=True)

    lane = lax.broadcasted_iota(jnp.int32, (1, HEAD_DIM), 1)
    lane_rows = lax.broadcasted_iota(jnp.int32, (1, rows), 1)
    small_eye = lax.broadcasted_iota(jnp.int32, (rows, rows), 0) == lax.broadcasted_iota(
        jnp.int32, (rows, rows), 1
    )

    def set_up():
        for copy in others:
            copy.wait()
        for i in range(heads_all):
            bias_rows[i : i + 1, :] = bias_v[:, i * HEAD_DIM : (i + 1) * HEAD_DIM].astype(F32)
        target = jnp.sum(
            jnp.where(small_eye, token_v[...].astype(F32), 0.0), axis=1, keepdims=True
        )
        target_v[...] = jnp.broadcast_to(target, target_v.shape)
        length = jnp.concatenate(
            [
                jnp.sum(
                    jnp.where(lane_rows == me * lc + i, len_v[...].astype(F32), 0.0),
                    axis=1,
                    keepdims=True,
                )
                for i in range(lc)
            ],
            axis=0,
        )
        angles = length * freq_v[...]
        cosines = jnp.cos(angles)
        sines = jnp.sin(angles) * jnp.where(lane < HEAD_DIM // 2, -1.0, 1.0)
        for i in range(lc):
            own = slice(i * group, (i + 1) * group)
            own_rows[own, :] = jnp.broadcast_to(length[i : i + 1], (group, HEAD_DIM))
            turn_cos[own, :] = jnp.broadcast_to(cosines[i : i + 1], (group, HEAD_DIM))
            turn_sin[own, :] = jnp.broadcast_to(sines[i : i + 1], (group, HEAD_DIM))

    def scale_rows():
        gain_copy.wait()
        current = x[...].astype(F32)
        sq[...] = jnp.broadcast_to(
            to_row(jnp.sum(current * current, axis=1, keepdims=True)), sq.shape
        )
        scaled[...] = (current * gain_v[...].astype(F32)).astype(BF16)

    def sq_copy(peer, slot):
        return remote(sq, sq_in.at[slot], sq_s, sq_r, (sec, peer))

    def sq_send():
        for k in far_first:
            sq_copy(to_peer(k), me).start()
        sq_in[me] = sq[...]

    def part_copy(phase, peer, slot):
        return remote(
            part.at[phase, peer],
            part_in.at[phase, slot],
            part_s,
            part_r.at[phase],
            (sec, peer),
        )

    def multiply(phase):
        wq_copy(phase).wait()
        base = pl.multiple_of(phase * cw, cw)
        piece = jnp.dot(scaled[...], wq[:, pl.ds(base, cw)], preferred_element_type=F32)
        for j in range(group):
            stage[pl.ds(j, rows, stride=group), :] = piece[
                :, j * HEAD_DIM : (j + 1) * HEAD_DIM
            ]
        for p in range(n):
            part[phase, p] = stage[p * span : (p + 1) * span, :].astype(BF16)

    def spread(phase):
        for k in far_first:
            part_copy(phase, to_peer(k), me).start()
        part_in[phase, me] = part[phase, me]

    def compute_only(k, carry):
        multiply(phase_of(k))
        return carry

    def send_only(k, carry):
        spread(phase_of(k))
        return carry

    def project(k, carry):
        multiply(phase_of(k))
        spread(phase_of(k))
        return carry

    def hop_copy(c, to):
        cols = pl.ds(c * chunk, chunk)
        return remote(xo.at[:, cols], x.at[:, cols], hop_s, hop_r, (to, me))


    @pl.when(sec == 0)
    def _():
        with jax.named_scope("hidden_wait"):
            hidden_copy.wait()
        scale_rows()
        wq_rest()
        for copy in others:
            copy.start()
        lax.fori_loop(0, early, compute_only, 0)

    @pl.when(sec > 0)
    def _():
        set_up()

    with jax.named_scope("barrier"):
        pl.semaphore_wait(barrier, n + sections - 2)

    @pl.when(sec == 0)
    def _():
        sq_send()
        lax.fori_loop(0, early, send_only, 0)

    @pl.when(sec > 0)
    def _():
        with jax.named_scope("hop_wait"):
            remote(xo, x, hop_s, hop_r, (sec - 1, me)).wait_recv()
        scale_rows()
        sq_send()

    lax.fori_loop(jnp.where(sec == 0, early, 0), phases, project, 0)

    @pl.when(sec == 0)
    def _():
        kv_copy.start()
        wo_copy.start()
        hw_copy.start()
        set_up()

    def summed(phase):
        with jax.named_scope("rs_wait"):
            remote(
                part.at[phase, pl.ds(1, n - 1)],
                part_in.at[phase, pl.ds(1, n - 1)],
                part_s,
                part_r.at[phase],
                (sec, me),
            ).wait_recv()
        result = part_in[phase, 0].astype(F32)
        for p in range(1, n):
            result = result + part_in[phase, p].astype(F32)
        return result

    with jax.named_scope("sq_wait"):
        remote(
            sq_in.at[pl.ds(1, n - 1)], sq_in.at[pl.ds(1, n - 1)], sq_s, sq_r, (sec, me)
        ).wait_recv()
    squares = sq_in[0]
    for p in range(1, n):
        squares = squares + sq_in[p]
    own_request = me * lc + lax.broadcasted_iota(jnp.int32, (span, 128), 0) // group
    own_lane = lax.broadcasted_iota(jnp.int32, (span, 128), 1)
    factor = lax.rsqrt(
        jnp.sum(jnp.where(own_lane == own_request, squares[0:1, :], 0.0), axis=1, keepdims=True)
        / (n * width)
        + EPS
    )
    pos = lax.broadcasted_iota(jnp.int32, (1, kv.shape[3]), 1).astype(F32)

    def turned(block):
        return block * turn_cos[...] + pltpu.roll(block, HEAD_DIM // 2, 1) * turn_sin[...]

    def each(rows_of):
        return jnp.concatenate([rows_of(i) for i in range(lc)], axis=0)

    def rows_at(i):
        return slice(i * group, (i + 1) * group)

    is_key = (
        lax.rem(lax.broadcasted_iota(jnp.int32, (span, HEAD_DIM), 0), 2 * KV_HEADS) < KV_HEADS
    )
    fresh_bias = bias_rows[HEADS:, :]
    block = summed(phases - 1) * factor + each(lambda i: fresh_bias)
    fresh[...] = jnp.where(is_key, turned(block), block).astype(BF16).astype(F32)
    kv_copy.wait()

    def att_copy(h, peer, slot):
        return remote(att.at[h], att_in.at[h, slot], att_s, att_r.at[h], (sec, peer))

    def attend(h, carry):
        block_sum = summed(h)
        with jax.named_scope("attend"):
            bias_h = bias_rows[pl.ds(pl.multiple_of(h * group, group), group), :]
            query = turned(block_sum * factor + each(lambda i: bias_h))
            scores = each(
                lambda i: lax.dot_general(
                    query[rows_at(i)].astype(BF16),
                    kv[i, 0, h],
                    (((1,), (1,)), ((), ())),
                    preferred_element_type=F32,
                )
            )
            scores = scores * scale
            repeat = lambda row: jnp.broadcast_to(fresh[pl.ds(row, 1), :], (group, HEAD_DIM))
            key_new = each(lambda i: repeat(i * group + h))
            value_new = each(lambda i: repeat(i * group + KV_HEADS + h))
            self_score = (
                jnp.sum(query.astype(BF16).astype(F32) * key_new, axis=1, keepdims=True) * scale
            )
            visible = pos < own_rows[:, 0:1]
            top = jnp.maximum(
                jnp.max(jnp.where(visible, scores, -1e30), axis=1, keepdims=True), self_score
            )
            weights = jnp.where(visible, jnp.exp(scores - top), 0.0)
            self_weight = jnp.exp(self_score - top)
            denominator = jnp.sum(weights, axis=1, keepdims=True) + self_weight
            mixed = each(
                lambda i: jnp.dot(
                    weights[rows_at(i)].astype(BF16), kv[i, 1, h], preferred_element_type=F32
                )
            )
            mixed = mixed + self_weight.astype(BF16).astype(F32) * value_new
            att[h] = (mixed / denominator).astype(BF16)
        for k in far_first:
            att_copy(h, to_peer(k), me).start()
        att_in[h, me] = att[h]
        return carry

    lax.fori_loop(0, KV_HEADS, attend, 0)
    wo_copy.wait()
    update[...] = x[...].astype(F32)

    def all_att(h):
        return remote(
            att_in.at[h, pl.ds(1, n - 1)],
            att_in.at[h, pl.ds(1, n - 1)],
            att_s,
            att_r.at[h],
            (sec, me),
        )

    def gathered(h):
        with jax.named_scope("ag_wait"):
            all_att(h).wait_recv()
        for p in range(n):
            stage[p * span : (p + 1) * span, :] = att_in[h, p].astype(F32)
        return jnp.concatenate(
            [stage[pl.ds(j, rows, stride=group), :].astype(BF16) for j in range(group)],
            axis=1,
        )

    def project_out(h, carry):
        mat = gathered(h)
        depth = pl.ds(pl.multiple_of(h * cw, cw), cw)
        update[...] += jnp.dot(mat, wo[depth, :], preferred_element_type=F32)
        return carry

    lax.fori_loop(0, KV_HEADS - 1, project_out, 0)

    def fin_copy(c, peer, slot):
        return remote(
            fin.at[core, slot, c],
            fin.at[core, slot, c],
            fin_s,
            fin_r.at[slot],
            (sec, peer),
        )

    def sib_copy(c, piece, slot):
        return remote(
            fin.at[piece, slot, c],
            fin.at[piece, slot, c],
            sib_s,
            sib_r.at[slot],
            (sibling, me),
        )

    def fsq_copy(peer, slot):
        return remote(
            fsq_in.at[slot], fsq_in.at[slot], fsq_s, fsq_r, (sec, peer)
        )

    def fp_copy(c, k):
        to = lax.rem(sec + k, sections)
        piece = lax.rem(to, 2)
        return remote(
            fin.at[piece, me, c], fin.at[piece, me, c], fp_s, fp_r.at[c], (to, me)
        )

    def fp_sq(k):
        to = lax.rem(sec + k, sections)
        return remote(
            fsq_in.at[me], fsq_in.at[me], fq_s, fp_r.at[chunks], (to, me)
        )

    mat = gathered(KV_HEADS - 1)
    top_rows = (KV_HEADS - 1) * cw
    final_sq = jnp.zeros((rows, 1), F32)
    for c in range(chunks):
        cols = slice(c * chunk, (c + 1) * chunk)
        grown = update[:, cols] + jnp.dot(
            mat, wo[top_rows : top_rows + cw, cols], preferred_element_type=F32
        )
        new = grown.astype(BF16)
        xo[:, cols] = new
        final = new.astype(F32)
        final_sq = final_sq + jnp.sum(final * final, axis=1, keepdims=True)

        @pl.when(sec < last)
        def _():
            hop_copy(c, sec + 1).start()

        @pl.when(sec == last)
        def _():
            lanes = chunk // 128
            row = jnp.concatenate(
                [final_v[c * lanes + i : c * lanes + i + 1, :].astype(F32) for i in range(lanes)],
                axis=1,
            )
            both = (final * row).astype(BF16)
            fin[0, me, c] = both[:half]
            fin[1, me, c] = both[half:]
            for k in range(1, sections):
                fp_copy(c, k).start()
            for k in far_first:
                fin_copy(c, to_peer(k), me).start()
            sib_copy(c, core, me).start()

    @pl.when(sec == last)
    def _():
        fsq_in[me] = to_row(final_sq)
        for k in range(1, sections):
            fp_sq(k).start()
        for k in far_first:
            fsq_copy(to_peer(k), me).start()

    @pl.when(sec < last)
    def _():
        for c in range(chunks):
            arriving = remote(
                fin.at[core, me, c], fin.at[core, me, c], fp_s, fp_r.at[c], (last, me)
            )
            with jax.named_scope("fp_wait"):
                arriving.wait_recv()
            for k in far_first:
                fin_copy(c, to_peer(k), me).start()

            @pl.when(sec < last - 1)
            def _():
                sib_copy(c, core, me).start()

        arriving = remote(
            fsq_in.at[me], fsq_in.at[me], fq_s, fp_r.at[chunks], (last, me)
        )
        arriving.wait_recv()
        for k in far_first:
            fsq_copy(to_peer(k), me).start()

    hw_copy.wait()

    def whole(piece, slot, send, recv):
        return remote(fin.at[piece, slot], fin.at[piece, slot], send, recv.at[slot], (sibling, me))

    def pass_on(k):
        _, peer = mate(me, k, n)
        with jax.named_scope("fin_wait"):
            whole(core, peer, fin_s, fin_r).wait_recv()
        for c in range(chunks):
            sib_copy(c, core, peer).start()

    def head(k, logits):
        _, peer = mate(me, k, n)
        if isinstance(k, int) and k == 0:

            @pl.when(sec < last)
            def _():
                whole(1 - core, peer, sib_s, sib_r).wait_recv()

        else:
            with jax.named_scope("sib_wait"):
                whole(1 - core, peer, sib_s, sib_r).wait_recv()
        for c in range(chunks):
            at = pl.ds(pl.multiple_of(peer * width + c * chunk, chunk), chunk)
            both = jnp.concatenate([fin[0, peer, c], fin[1, peer, c]], axis=0)
            logits = logits + jnp.dot(both, hw[at, :], preferred_element_type=F32)
        return logits

    lag = min(2, n - 1)
    for k in range(1, lag + 1):
        pass_on(k)
    logits = head(0, jnp.zeros(out.shape, F32))

    def step(k, logits):
        pass_on(k)
        return head(k - lag, logits)

    logits = lax.fori_loop(lag + 1, n, step, logits)
    logits = lax.fori_loop(n - lag, n, head, logits)
    all_fsq = remote(
        fsq_in.at[pl.ds(1, n - 1)], fsq_in.at[pl.ds(1, n - 1)], fsq_s, fsq_r, (sec, me)
    )
    all_fsq.wait_recv()
    squares = jnp.sum(fsq_in[:, 0, :], axis=0, keepdims=True)
    logits = logits * lax.rsqrt(to_col(squares) / (n * width) + EPS)
    vocab = out.shape[1]
    ids = (mine * vocab + lax.broadcasted_iota(jnp.int32, (1, vocab), 1)).astype(F32)
    picked = jnp.sum(jnp.where(ids == target_v[:, 0:1], logits, 0.0), axis=1, keepdims=True)
    top = jnp.max(logits, axis=1, keepdims=True)
    amount = jnp.sum(jnp.exp(logits - top), axis=1, keepdims=True)
    row_of = lax.broadcasted_iota(jnp.int32, (rows, 128), 0)
    lane_of = lax.broadcasted_iota(jnp.int32, (rows, 128), 1)
    packed = jnp.where(lane_of == row_of, top, 0.0)
    packed = jnp.where(lane_of == row_of + rows, amount, packed)
    packed = jnp.where(lane_of == row_of + 2 * rows, picked, packed)
    red[...] = jnp.sum(packed, axis=0, keepdims=True)

    def red_copy(other, slot):
        return remote(
            red, red_in.at[slot], red_s, red_r, (other // n, lax.rem(other, n))
        )

    if total <= 64:
        for k in range(total - 1, 0, -1):
            red_copy(mate(mine, k, total)[0], mine).start()
    else:

        def red_start(k, carry):
            red_copy(mate(mine, total - k, total)[0], mine).start()
            return carry

        lax.fori_loop(1, total, red_start, 0)
    red_in[mine] = red[...]
    flat[...] = logits

    def sent(ref, sem):
        remote(ref, ref, sem, sem, (sec, me)).wait_send()

    others_n = pl.ds(1, n - 1)
    sent(sq_in.at[others_n], sq_s)
    sent(part_in.at[:, others_n], part_s)
    sent(att_in.at[:, others_n], att_s)
    sent(fin.at[0, others_n], fin_s)
    sent(fin.at[0, others_n], sib_s)
    all_fsq.wait_send()

    @pl.when(sec != last - 1)
    def _():
        sent(fin.at[0, 0], sib_s)

    @pl.when(sec < last)
    def _():
        sent(xo, hop_s)

    @pl.when(sec == last)
    def _():
        sent(fin.at[0, pl.ds(1, sections - 1)], fp_s)
        sent(fsq_in.at[pl.ds(1, sections - 1)], fq_s)

    order = (
        jnp.sum(jnp.where(small_eye, slot_v[...].astype(F32), 0.0), axis=1, keepdims=True)
        == lane_of.astype(F32)
    )
    for s in range(rows):
        out[s : s + 1, :] = flat[pl.ds(slot_s[0, s], 1), :]

    everyone = remote(
        red_in.at[pl.ds(1, total - 1)],
        red_in.at[pl.ds(1, total - 1)],
        red_s,
        red_r,
        (sec, me),
    )
    with jax.named_scope("red_wait"):
        everyone.wait_recv()
    seen = red_in[:, 0, :]
    row_top = jnp.max(seen, axis=0, keepdims=True)
    amounts = pltpu.roll(seen, 128 - rows, 1)
    row_total = jnp.sum(amounts * jnp.exp(jnp.minimum(seen - row_top, 0.0)), axis=0, keepdims=True)
    log_total = row_top + jnp.log(row_total)
    total_col = jnp.sum(jnp.where(order, log_total, 0.0), axis=1, keepdims=True)
    out[...] = out[...] - total_col
    scored = pltpu.roll(jnp.sum(seen, axis=0, keepdims=True), 128 - 2 * rows, 1) - log_total
    chosen[...] = to_row(jnp.sum(jnp.where(order, scored, 0.0), axis=1, keepdims=True))
    with jax.named_scope("red_sent"):
        everyone.wait_send()


def local(
    hidden_in,
    lengths,
    assign,
    token_ids,
    attn_gain,
    qkv_weight,
    qkv_bias,
    out_weight,
    kv_cache,
    final_gain,
    head_weight,
):
    sections = lax.axis_size("pipe")
    n = lax.axis_size("mp")
    rows, width = hidden_in.shape
    lc = kv_cache.shape[1]
    qkv = qkv_weight.shape[2]
    inner = out_weight.shape[1]
    vocab = head_weight.shape[1]
    heads_all = HEADS + 2 * KV_HEADS
    half = HEAD_DIM // 2
    frequency = np.float32(THETA) ** (
        -np.arange(half).astype(np.float32) * np.float32(2.0) / np.float32(HEAD_DIM)
    )
    freq = jnp.asarray(np.concatenate([frequency, frequency])[None, :], F32)
    group = HEADS // KV_HEADS
    phases = heads_all // group
    span = lc * group
    dma = pltpu.SemaphoreType.DMA
    vm = pl.BlockSpec(memory_space=pltpu.VMEM)
    hbm = pl.BlockSpec(memory_space=pltpu.HBM)
    total = sections * n
    chunks = 2
    logprobs, chosen = pl.pallas_call(
        functools.partial(kernel, sections, n),
        out_shape=(
            jax.ShapeDtypeStruct((rows, vocab), F32),
            jax.ShapeDtypeStruct((1, 128), F32),
        ),
        in_specs=[hbm] * 12,
        out_specs=(vm, vm),
        scratch_shapes=[
            pltpu.VMEM((width, qkv), BF16),
            pltpu.VMEM((inner, width), BF16),
            pltpu.VMEM(kv_cache.shape[1:], BF16),
            pltpu.VMEM(head_weight.shape, BF16),
            pltpu.VMEM((rows, width), BF16),
            pltpu.VMEM((rows, width), BF16),
            pltpu.VMEM((rows, width), BF16),
            pltpu.VMEM((rows * group, HEAD_DIM), F32),
            pltpu.VMEM((phases, n, span, HEAD_DIM), BF16),
            pltpu.VMEM((phases, n, span, HEAD_DIM), BF16),
            pltpu.VMEM((8, 128), F32),
            pltpu.VMEM((n, 8, 128), F32),
            pltpu.VMEM((1, width), BF16),
            pltpu.VMEM((1, qkv), BF16),
            pltpu.VMEM((width // 128, 128), BF16),
            pltpu.VMEM((1, rows), jnp.int32),
            pltpu.VMEM((1, rows), jnp.int32),
            pltpu.VMEM((1, rows), jnp.int32),
            pltpu.VMEM((1, HEAD_DIM), F32),
            pltpu.SMEM((1, rows), jnp.int32),
            pltpu.VMEM((heads_all, HEAD_DIM), F32),
            pltpu.VMEM((span, HEAD_DIM), F32),
            pltpu.VMEM((span, HEAD_DIM), F32),
            pltpu.VMEM((span, HEAD_DIM), F32),
            pltpu.VMEM((rows, 128), F32),
            pltpu.VMEM((span, HEAD_DIM), F32),
            pltpu.VMEM((KV_HEADS, span, HEAD_DIM), BF16),
            pltpu.VMEM((KV_HEADS, n, span, HEAD_DIM), BF16),
            pltpu.VMEM((rows, width), F32),
            pltpu.VMEM((2, n, chunks, rows // 2, width // chunks), BF16),
            pltpu.VMEM((n, 1, 128), F32),
            pltpu.VMEM((1, 128), F32),
            pltpu.VMEM((total, 1, 128), F32),
            pltpu.VMEM((rows, vocab), F32),
            dma((phases,)),
            dma((3,)),
            dma((9,)),
            dma,
            dma((phases,)),
            dma,
            dma,
            dma,
            dma((KV_HEADS,)),
            dma,
            dma,
            dma,
            dma((n,)),
            dma,
            dma((n,)),
            dma,
            dma,
            dma,
            dma,
            dma((chunks + 1,)),
            dma,
            dma,
        ],
        compiler_params=pltpu.CompilerParams(
            collective_id=0, has_side_effects=True, vmem_limit_bytes=60 * 1024 * 1024
        ),
    )(
        hidden_in,
        lengths.reshape(1, rows),
        assign.reshape(1, rows),
        token_ids.reshape(1, rows),
        attn_gain,
        qkv_weight,
        qkv_bias,
        out_weight,
        kv_cache,
        final_gain.reshape(width // 128, 128),
        head_weight,
        freq,
    )
    return logprobs, chosen[0, :rows]


def solution(mesh):
    return jax.shard_map(
        local,
        mesh=mesh,
        in_specs=(
            P(None, "mp"),
            P(),
            P(),
            P(),
            P("pipe", "mp"),
            P("pipe", "mp", None),
            P("pipe", None),
            P("pipe", None, "mp"),
            P("pipe", "mp", None, None, None, None),
            P("mp"),
            P(None, ("pipe", "mp")),
        ),
        out_specs=(P(None, ("pipe", "mp")), P()),
        check_vma=False,
    )
```

```python
import functools

import jax
import jax.numpy as jnp
import numpy as np
from jax import lax
from jax.experimental import pallas as pl
from jax.experimental.pallas import tpu as pltpu
from jax.sharding import PartitionSpec as P

HEADS = 32
KV_HEADS = 4
HEAD_DIM = 128
EPS = 1e-06
THETA = 1000000.0
MESH = pl.DeviceIdType.MESH
F32 = jnp.float32
BF16 = jnp.bfloat16


def remote(src, dst, send_sem, recv_sem, device):
    return pltpu.make_async_remote_copy(
        src_ref=src,
        dst_ref=dst,
        send_sem=send_sem,
        recv_sem=recv_sem,
        device_id=device,
        device_id_type=MESH,
    )


def kernel(
    sections,
    n,
    hidden,
    lengths,
    assign,
    token_ids,
    gain,
    qkv_weight,
    bias,
    out_weight,
    cache,
    final_gain,
    head_weight,
    freq,
    out,
    chosen,
    wq,
    wo,
    kv,
    hw,
    x,
    xo,
    scaled,
    stage,
    part,
    part_in,
    sq,
    sq_in,
    gain_v,
    bias_v,
    final_v,
    len_v,
    slot_v,
    token_v,
    freq_v,
    slot_s,
    bias_rows,
    turn_cos,
    turn_sin,
    own_rows,
    target_v,
    fresh,
    att,
    att_in,
    update,
    fin,
    fsq_in,
    red,
    red_in,
    flat,
    wq_sem,
    w_sem,
    small_sem,
    part_s,
    part_r,
    sq_s,
    sq_r,
    att_s,
    att_r,
    hop_s,
    hop_r,
    fin_s,
    fin_r,
    sib_s,
    sib_r,
    fsq_s,
    fsq_r,
    fp_s,
    fq_s,
    fp_r,
    red_s,
    red_r,
    help_s,
    help_r,
):
    sec = lax.axis_index("pipe")
    me = lax.axis_index("mp")
    total = sections * n
    rows, width = x.shape
    lc = kv.shape[1]
    heads_all = HEADS + 2 * KV_HEADS
    group = HEADS // KV_HEADS
    phases = heads_all // group
    span = lc * group
    last = sections - 1
    scale = HEAD_DIM ** (-0.5)
    cw = group * HEAD_DIM
    half = rows // 2
    chunks = fin.shape[2]
    chunk = width // chunks
    core = lax.rem(sec, 2)
    sibling = sec + 1 - 2 * core
    mine = sec * n + me
    runs = (sec < 2) | (core == 1)
    helps = (sec >= 2) & (core == 0)
    helped = (sec >= 2) & (core == 1)
    following = jnp.where(sec == 0, 1, sec + 2)
    early = min(2, phases)

    def mate(own, k, count):
        if count & (count - 1):
            return lax.rem(own + k, count), lax.rem(own + count - k, count)
        other = 0
        for b in range(count.bit_length() - 1):
            place = 1 << b
            mine_bit = lax.rem(own // place, 2)
            if isinstance(k, int):
                bit = 1 - mine_bit if (k // place) % 2 else mine_bit
            else:
                flip = lax.rem(k // place, 2)
                bit = mine_bit + flip - 2 * mine_bit * flip
            other = other + place * bit
        return other, other

    pairs = [mate(me, k, n) for k in range(n)]
    far_first = range(n - 1, 0, -1)

    def to_peer(k):
        return pairs[k][0]

    def from_peer(k):
        return pairs[k][1]

    def wq_copy(c):
        cols = pl.ds(pl.multiple_of(c * cw, cw), cw)
        return pltpu.make_async_copy(qkv_weight.at[0, :, cols], wq.at[1, :, cols], wq_sem.at[c])

    def phase_of(k):
        return lax.rem(k + phases - 1, phases)

    def small(i, src, dst):
        return pltpu.make_async_copy(src, dst, small_sem.at[i])

    hidden_copy = small(0, hidden, x)
    gain_copy = small(1, gain, gain_v.at[1])
    others = [
        small(2, bias, bias_v.at[1]),
        small(3, final_gain, final_v),
        small(4, lengths, len_v),
        small(5, assign, slot_v),
        small(6, token_ids, token_v),
        small(7, freq, freq_v),
        small(8, assign, slot_s),
    ]

    @pl.when(sec == 0)
    def _():
        hidden_copy.start()

    @pl.when(runs)
    def _():
        gain_copy.start()
        for k in range(early):
            wq_copy((k + phases - 1) % phases).start()

    def wq_rest():
        for k in range(early, phases):
            wq_copy((k + phases - 1) % phases).start()

    kv_copy = pltpu.make_async_copy(cache.at[0], kv.at[1], w_sem.at[0])
    wo_copy = pltpu.make_async_copy(out_weight.at[0], wo.at[1], w_sem.at[1])
    hw_copy = pltpu.make_async_copy(head_weight, hw, w_sem.at[2])

    barrier = pltpu.get_barrier_semaphore()
    for k in far_first:
        pl.semaphore_signal(barrier, inc=1, device_id=(sec, to_peer(k)), device_id_type=MESH)
    for k in range(1, sections):
        pl.semaphore_signal(
            barrier, inc=1, device_id=(lax.rem(sec + k, sections), me), device_id_type=MESH
        )
    @pl.when(sec > 0)
    def _():
        for copy in others:
            copy.start()
        hw_copy.start()

    @pl.when((sec > 0) & runs)
    def _():
        wq_rest()
        kv_copy.start()
        wo_copy.start()

    def help_copy(i, src, dst):
        return remote(src, dst, help_s, help_r.at[i], (sibling, me))

    help_copies = [
        help_copy(0, gain, gain_v.at[0]),
        help_copy(1, bias, bias_v.at[0]),
        help_copy(2, qkv_weight.at[0], wq.at[0]),
        help_copy(3, cache.at[0], kv.at[0]),
        help_copy(4, out_weight.at[0], wo.at[0]),
    ]

    eye = lax.broadcasted_iota(jnp.int32, (rows, 128), 0) == lax.broadcasted_iota(
        jnp.int32, (rows, 128), 1
    )

    def to_row(col):
        return jnp.sum(jnp.where(eye, col, 0.0), axis=0, keepdims=True)

    def to_col(row):
        return jnp.sum(jnp.where(eye, row, 0.0), axis=1, keepdims=True)

    lane = lax.broadcasted_iota(jnp.int32, (1, HEAD_DIM), 1)
    lane_rows = lax.broadcasted_iota(jnp.int32, (1, rows), 1)
    small_eye = lax.broadcasted_iota(jnp.int32, (rows, rows), 0) == lax.broadcasted_iota(
        jnp.int32, (rows, rows), 1
    )

    def set_bias(t):
        for i in range(heads_all):
            bias_rows[t, i : i + 1, :] = bias_v[
                t, :, i * HEAD_DIM : (i + 1) * HEAD_DIM
            ].astype(F32)

    def set_up():
        for copy in others:
            copy.wait()
        set_bias(1)
        target = jnp.sum(
            jnp.where(small_eye, token_v[...].astype(F32), 0.0), axis=1, keepdims=True
        )
        target_v[...] = jnp.broadcast_to(target, target_v.shape)
        length = jnp.concatenate(
            [
                jnp.sum(
                    jnp.where(lane_rows == me * lc + i, len_v[...].astype(F32), 0.0),
                    axis=1,
                    keepdims=True,
                )
                for i in range(lc)
            ],
            axis=0,
        )
        angles = length * freq_v[...]
        cosines = jnp.cos(angles)
        sines = jnp.sin(angles) * jnp.where(lane < HEAD_DIM // 2, -1.0, 1.0)
        for i in range(lc):
            own = slice(i * group, (i + 1) * group)
            own_rows[own, :] = jnp.broadcast_to(length[i : i + 1], (group, HEAD_DIM))
            turn_cos[own, :] = jnp.broadcast_to(cosines[i : i + 1], (group, HEAD_DIM))
            turn_sin[own, :] = jnp.broadcast_to(sines[i : i + 1], (group, HEAD_DIM))

    def scale_rows(t):
        current = x[...].astype(F32)
        sq[t] = jnp.broadcast_to(
            to_row(jnp.sum(current * current, axis=1, keepdims=True)), sq.shape[1:]
        )
        scaled[...] = (current * gain_v[t].astype(F32)).astype(BF16)

    def sq_copy(t, peer, slot):
        return remote(sq.at[t], sq_in.at[t, slot], sq_s.at[t], sq_r.at[t], (sec, peer))

    def sq_send(t):
        for k in far_first:
            sq_copy(t, to_peer(k), me).start()
        sq_in[t, me] = sq[t]

    def part_copy(t, phase, peer, slot):
        return remote(
            part.at[t, phase, peer],
            part_in.at[t, phase, slot],
            part_s.at[t],
            part_r.at[t, phase],
            (sec, peer),
        )

    def multiply(t, phase):
        if t == 1:
            wq_copy(phase).wait()
        base = pl.multiple_of(phase * cw, cw)
        piece = jnp.dot(scaled[...], wq[t, :, pl.ds(base, cw)], preferred_element_type=F32)
        for j in range(group):
            stage[pl.ds(j, rows, stride=group), :] = piece[
                :, j * HEAD_DIM : (j + 1) * HEAD_DIM
            ]
        for p in range(n):
            part[t, phase, p] = stage[p * span : (p + 1) * span, :].astype(BF16)

    def spread(t, phase):
        for k in far_first:
            part_copy(t, phase, to_peer(k), me).start()
        part_in[t, phase, me] = part[t, phase, me]

    def compute_only(k, carry):
        multiply(1, phase_of(k))
        return carry

    def send_only(k, carry):
        spread(1, phase_of(k))
        return carry

    def project(t):
        def one(k, carry):
            multiply(t, phase_of(k))
            spread(t, phase_of(k))
            return carry

        return one

    def hop_copy(c, to):
        cols = pl.ds(c * chunk, chunk)
        return remote(xo.at[:, cols], x.at[:, cols], hop_s, hop_r, (to, me))


    @pl.when(sec == 0)
    def _():
        with jax.named_scope("hidden_wait"):
            hidden_copy.wait()
        gain_copy.wait()
        scale_rows(1)
        wq_rest()
        for copy in others:
            copy.start()
        lax.fori_loop(0, early, compute_only, 0)

    @pl.when(sec > 0)
    def _():
        set_up()

    with jax.named_scope("barrier"):
        pl.semaphore_wait(barrier, n + sections - 2)

    @pl.when(helps)
    def _():
        for copy in help_copies:
            copy.start()

    pos = lax.broadcasted_iota(jnp.int32, (1, kv.shape[4]), 1).astype(F32)
    own_request = me * lc + lax.broadcasted_iota(jnp.int32, (span, 128), 0) // group
    own_lane = lax.broadcasted_iota(jnp.int32, (span, 128), 1)
    is_key = (
        lax.rem(lax.broadcasted_iota(jnp.int32, (span, HEAD_DIM), 0), 2 * KV_HEADS) < KV_HEADS
    )

    def turned(block):
        return block * turn_cos[...] + pltpu.roll(block, HEAD_DIM // 2, 1) * turn_sin[...]

    def each(rows_of):
        return jnp.concatenate([rows_of(i) for i in range(lc)], axis=0)

    def rows_at(i):
        return slice(i * group, (i + 1) * group)

    def att_copy(t, h, peer, slot):
        return remote(
            att.at[t, h], att_in.at[t, h, slot], att_s.at[t], att_r.at[t, h], (sec, peer)
        )

    def all_att(t, h):
        return remote(
            att_in.at[t, h, pl.ds(1, n - 1)],
            att_in.at[t, h, pl.ds(1, n - 1)],
            att_s.at[t],
            att_r.at[t, h],
            (sec, me),
        )

    def summed(t, phase):
        with jax.named_scope("rs_wait"):
            remote(
                part.at[t, phase, pl.ds(1, n - 1)],
                part_in.at[t, phase, pl.ds(1, n - 1)],
                part_s.at[t],
                part_r.at[t, phase],
                (sec, me),
            ).wait_recv()
        result = part_in[t, phase, 0].astype(F32)
        for p in range(1, n):
            result = result + part_in[t, phase, p].astype(F32)
        return result

    def attention(t):
        with jax.named_scope("sq_wait"):
            remote(
                sq_in.at[t, pl.ds(1, n - 1)],
                sq_in.at[t, pl.ds(1, n - 1)],
                sq_s.at[t],
                sq_r.at[t],
                (sec, me),
            ).wait_recv()
        squares = sq_in[t, 0]
        for p in range(1, n):
            squares = squares + sq_in[t, p]
        factor = lax.rsqrt(
            jnp.sum(
                jnp.where(own_lane == own_request, squares[0:1, :], 0.0), axis=1, keepdims=True
            )
            / (n * width)
            + EPS
        )
        fresh_bias = bias_rows[t, HEADS:, :]
        block = summed(t, phases - 1) * factor + each(lambda i: fresh_bias)
        fresh[...] = jnp.where(is_key, turned(block), block).astype(BF16).astype(F32)
        if t == 1:
            kv_copy.wait()
        else:
            help_copies[3].wait_recv()

        def attend(h, carry):
            block_sum = summed(t, h)
            with jax.named_scope("attend"):
                bias_h = bias_rows[t, pl.ds(pl.multiple_of(h * group, group), group), :]
                query = turned(block_sum * factor + each(lambda i: bias_h))
                scores = each(
                    lambda i: lax.dot_general(
                        query[rows_at(i)].astype(BF16),
                        kv[t, i, 0, h],
                        (((1,), (1,)), ((), ())),
                        preferred_element_type=F32,
                    )
                )
                scores = scores * scale
                repeat = lambda row: jnp.broadcast_to(
                    fresh[pl.ds(row, 1), :], (group, HEAD_DIM)
                )
                key_new = each(lambda i: repeat(i * group + h))
                value_new = each(lambda i: repeat(i * group + KV_HEADS + h))
                self_score = (
                    jnp.sum(query.astype(BF16).astype(F32) * key_new, axis=1, keepdims=True)
                    * scale
                )
                visible = pos < own_rows[:, 0:1]
                top = jnp.maximum(
                    jnp.max(jnp.where(visible, scores, -1e30), axis=1, keepdims=True),
                    self_score,
                )
                weights = jnp.where(visible, jnp.exp(scores - top), 0.0)
                self_weight = jnp.exp(self_score - top)
                denominator = jnp.sum(weights, axis=1, keepdims=True) + self_weight
                mixed = each(
                    lambda i: jnp.dot(
                        weights[rows_at(i)].astype(BF16),
                        kv[t, i, 1, h],
                        preferred_element_type=F32,
                    )
                )
                mixed = mixed + self_weight.astype(BF16).astype(F32) * value_new
                att[t, h] = (mixed / denominator).astype(BF16)
            for k in far_first:
                att_copy(t, h, to_peer(k), me).start()
            att_in[t, h, me] = att[t, h]
            return carry

        lax.fori_loop(0, KV_HEADS, attend, 0)
        if t == 1:
            wo_copy.wait()
        else:
            help_copies[4].wait_recv()
        update[...] = x[...].astype(F32)

        def project_out(h, carry):
            mat = gathered(t, h)
            depth = pl.ds(pl.multiple_of(h * cw, cw), cw)
            update[...] += jnp.dot(mat, wo[t, depth, :], preferred_element_type=F32)
            return carry

        lax.fori_loop(0, KV_HEADS - 1, project_out, 0)

    def gathered(t, h):
        with jax.named_scope("ag_wait"):
            all_att(t, h).wait_recv()
        for p in range(n):
            stage[p * span : (p + 1) * span, :] = att_in[t, h, p].astype(F32)
        return jnp.concatenate(
            [stage[pl.ds(j, rows, stride=group), :].astype(BF16) for j in range(group)],
            axis=1,
        )

    top_rows = (KV_HEADS - 1) * cw

    def grown(t, mat, cols):
        return (
            update[:, cols]
            + jnp.dot(
                mat, wo[t, top_rows : top_rows + cw, cols], preferred_element_type=F32
            )
        ).astype(BF16)

    @pl.when(sec == 0)
    def _():
        sq_send(1)
        lax.fori_loop(0, early, send_only, 0)

    @pl.when(core == 1)
    def _():
        gain_copy.wait()
        with jax.named_scope("hop_wait"):
            remote(xo, x, hop_s, hop_r, (sec - 1, me)).wait_recv()

    @pl.when(helped)
    def _():
        help_copies[0].wait_recv()
        help_copies[1].wait_recv()
        help_copies[2].wait_recv()
        scale_rows(0)
        sq_send(0)
        lax.fori_loop(0, phases, project(0), 0)
        set_bias(0)
        attention(0)
        x[...] = grown(0, gathered(0, KV_HEADS - 1), slice(0, width))

    @pl.when(core == 1)
    def _():
        scale_rows(1)
        sq_send(1)

    @pl.when(runs)
    def _():
        lax.fori_loop(jnp.where(sec == 0, early, 0), phases, project(1), 0)

    @pl.when(sec == 0)
    def _():
        kv_copy.start()
        wo_copy.start()
        hw_copy.start()
        set_up()

    def fin_copy(c, peer, slot):
        return remote(
            fin.at[core, slot, c],
            fin.at[core, slot, c],
            fin_s,
            fin_r.at[slot],
            (sec, peer),
        )

    def sib_copy(c, piece, slot):
        return remote(
            fin.at[piece, slot, c],
            fin.at[piece, slot, c],
            sib_s,
            sib_r.at[slot],
            (sibling, me),
        )

    def fsq_copy(peer, slot):
        return remote(
            fsq_in.at[slot], fsq_in.at[slot], fsq_s, fsq_r, (sec, peer)
        )

    def fp_copy(c, k):
        to = lax.rem(sec + k, sections)
        piece = lax.rem(to, 2)
        return remote(
            fin.at[piece, me, c], fin.at[piece, me, c], fp_s, fp_r.at[c], (to, me)
        )

    def fp_sq(k):
        to = lax.rem(sec + k, sections)
        return remote(
            fsq_in.at[me], fsq_in.at[me], fq_s, fp_r.at[chunks], (to, me)
        )

    @pl.when(runs)
    def _():
        attention(1)
        mat = gathered(1, KV_HEADS - 1)
        final_sq = jnp.zeros((rows, 1), F32)
        for c in range(chunks):
            cols = slice(c * chunk, (c + 1) * chunk)
            new = grown(1, mat, cols)
            xo[:, cols] = new
            final = new.astype(F32)
            final_sq = final_sq + jnp.sum(final * final, axis=1, keepdims=True)

            @pl.when(sec < last)
            def _():
                hop_copy(c, following).start()

            @pl.when(sec == last)
            def _():
                lanes = chunk // 128
                row = jnp.concatenate(
                    [
                        final_v[c * lanes + i : c * lanes + i + 1, :].astype(F32)
                        for i in range(lanes)
                    ],
                    axis=1,
                )
                both = (final * row).astype(BF16)
                fin[0, me, c] = both[:half]
                fin[1, me, c] = both[half:]
                for k in range(1, sections):
                    fp_copy(c, k).start()
                for k in far_first:
                    fin_copy(c, to_peer(k), me).start()
                sib_copy(c, core, me).start()

        @pl.when(sec == last)
        def _():
            fsq_in[me] = to_row(final_sq)
            for k in range(1, sections):
                fp_sq(k).start()
            for k in far_first:
                fsq_copy(to_peer(k), me).start()

    @pl.when(sec < last)
    def _():
        for c in range(chunks):
            arriving = remote(
                fin.at[core, me, c], fin.at[core, me, c], fp_s, fp_r.at[c], (last, me)
            )
            with jax.named_scope("fp_wait"):
                arriving.wait_recv()
            for k in far_first:
                fin_copy(c, to_peer(k), me).start()

            @pl.when(sec < last - 1)
            def _():
                sib_copy(c, core, me).start()

        arriving = remote(
            fsq_in.at[me], fsq_in.at[me], fq_s, fp_r.at[chunks], (last, me)
        )
        arriving.wait_recv()
        for k in far_first:
            fsq_copy(to_peer(k), me).start()

    hw_copy.wait()

    def whole(piece, slot, send, recv):
        return remote(fin.at[piece, slot], fin.at[piece, slot], send, recv.at[slot], (sibling, me))

    def pass_on(k):
        _, peer = mate(me, k, n)
        with jax.named_scope("fin_wait"):
            whole(core, peer, fin_s, fin_r).wait_recv()
        for c in range(chunks):
            sib_copy(c, core, peer).start()

    def head(k, logits):
        _, peer = mate(me, k, n)
        if isinstance(k, int) and k == 0:

            @pl.when(sec < last)
            def _():
                whole(1 - core, peer, sib_s, sib_r).wait_recv()

        else:
            with jax.named_scope("sib_wait"):
                whole(1 - core, peer, sib_s, sib_r).wait_recv()
        for c in range(chunks):
            at = pl.ds(pl.multiple_of(peer * width + c * chunk, chunk), chunk)
            both = jnp.concatenate([fin[0, peer, c], fin[1, peer, c]], axis=0)
            logits = logits + jnp.dot(both, hw[at, :], preferred_element_type=F32)
        return logits

    lag = min(2, n - 1)
    for k in range(1, lag + 1):
        pass_on(k)
    logits = head(0, jnp.zeros(out.shape, F32))

    def step(k, logits):
        pass_on(k)
        return head(k - lag, logits)

    logits = lax.fori_loop(lag + 1, n, step, logits)
    logits = lax.fori_loop(n - lag, n, head, logits)
    all_fsq = remote(
        fsq_in.at[pl.ds(1, n - 1)], fsq_in.at[pl.ds(1, n - 1)], fsq_s, fsq_r, (sec, me)
    )
    all_fsq.wait_recv()
    squares = jnp.sum(fsq_in[:, 0, :], axis=0, keepdims=True)
    logits = logits * lax.rsqrt(to_col(squares) / (n * width) + EPS)
    vocab = out.shape[1]
    ids = (mine * vocab + lax.broadcasted_iota(jnp.int32, (1, vocab), 1)).astype(F32)
    picked = jnp.sum(jnp.where(ids == target_v[:, 0:1], logits, 0.0), axis=1, keepdims=True)
    top = jnp.max(logits, axis=1, keepdims=True)
    amount = jnp.sum(jnp.exp(logits - top), axis=1, keepdims=True)
    row_of = lax.broadcasted_iota(jnp.int32, (rows, 128), 0)
    lane_of = lax.broadcasted_iota(jnp.int32, (rows, 128), 1)
    packed = jnp.where(lane_of == row_of, top, 0.0)
    packed = jnp.where(lane_of == row_of + rows, amount, packed)
    packed = jnp.where(lane_of == row_of + 2 * rows, picked, packed)
    red[...] = jnp.sum(packed, axis=0, keepdims=True)

    def red_copy(other, slot):
        return remote(
            red, red_in.at[slot], red_s, red_r, (other // n, lax.rem(other, n))
        )

    if total <= 64:
        for k in range(total - 1, 0, -1):
            red_copy(mate(mine, k, total)[0], mine).start()
    else:

        def red_start(k, carry):
            red_copy(mate(mine, total - k, total)[0], mine).start()
            return carry

        lax.fori_loop(1, total, red_start, 0)
    red_in[mine] = red[...]
    flat[...] = logits

    def sent(ref, sem):
        remote(ref, ref, sem, sem, (sec, me)).wait_send()

    others_n = pl.ds(1, n - 1)

    def stage_sent(t):
        sent(sq_in.at[t, others_n], sq_s.at[t])
        sent(part_in.at[t, :, others_n], part_s.at[t])
        sent(att_in.at[t, :, others_n], att_s.at[t])

    @pl.when(helped)
    def _():
        stage_sent(0)

    @pl.when(runs)
    def _():
        stage_sent(1)

    @pl.when(helps)
    def _():
        for copy in help_copies:
            copy.wait_send()

    sent(fin.at[0, others_n], fin_s)
    sent(fin.at[0, others_n], sib_s)
    all_fsq.wait_send()

    @pl.when(sec != last - 1)
    def _():
        sent(fin.at[0, 0], sib_s)

    @pl.when((sec < last) & runs)
    def _():
        sent(xo, hop_s)

    @pl.when(sec == last)
    def _():
        sent(fin.at[0, pl.ds(1, sections - 1)], fp_s)
        sent(fsq_in.at[pl.ds(1, sections - 1)], fq_s)

    order = (
        jnp.sum(jnp.where(small_eye, slot_v[...].astype(F32), 0.0), axis=1, keepdims=True)
        == lane_of.astype(F32)
    )
    for s in range(rows):
        out[s : s + 1, :] = flat[pl.ds(slot_s[0, s], 1), :]

    everyone = remote(
        red_in.at[pl.ds(1, total - 1)],
        red_in.at[pl.ds(1, total - 1)],
        red_s,
        red_r,
        (sec, me),
    )
    with jax.named_scope("red_wait"):
        everyone.wait_recv()
    seen = red_in[:, 0, :]
    row_top = jnp.max(seen, axis=0, keepdims=True)
    amounts = pltpu.roll(seen, 128 - rows, 1)
    row_total = jnp.sum(amounts * jnp.exp(jnp.minimum(seen - row_top, 0.0)), axis=0, keepdims=True)
    log_total = row_top + jnp.log(row_total)
    total_col = jnp.sum(jnp.where(order, log_total, 0.0), axis=1, keepdims=True)
    out[...] = out[...] - total_col
    scored = pltpu.roll(jnp.sum(seen, axis=0, keepdims=True), 128 - 2 * rows, 1) - log_total
    chosen[...] = to_row(jnp.sum(jnp.where(order, scored, 0.0), axis=1, keepdims=True))
    with jax.named_scope("red_sent"):
        everyone.wait_send()


def local(
    hidden_in,
    lengths,
    assign,
    token_ids,
    attn_gain,
    qkv_weight,
    qkv_bias,
    out_weight,
    kv_cache,
    final_gain,
    head_weight,
):
    sections = lax.axis_size("pipe")
    n = lax.axis_size("mp")
    rows, width = hidden_in.shape
    lc = kv_cache.shape[1]
    qkv = qkv_weight.shape[2]
    inner = out_weight.shape[1]
    vocab = head_weight.shape[1]
    heads_all = HEADS + 2 * KV_HEADS
    half = HEAD_DIM // 2
    frequency = np.float32(THETA) ** (
        -np.arange(half).astype(np.float32) * np.float32(2.0) / np.float32(HEAD_DIM)
    )
    freq = jnp.asarray(np.concatenate([frequency, frequency])[None, :], F32)
    group = HEADS // KV_HEADS
    phases = heads_all // group
    span = lc * group
    dma = pltpu.SemaphoreType.DMA
    vm = pl.BlockSpec(memory_space=pltpu.VMEM)
    hbm = pl.BlockSpec(memory_space=pltpu.HBM)
    total = sections * n
    chunks = 2
    logprobs, chosen = pl.pallas_call(
        functools.partial(kernel, sections, n),
        out_shape=(
            jax.ShapeDtypeStruct((rows, vocab), F32),
            jax.ShapeDtypeStruct((1, 128), F32),
        ),
        in_specs=[hbm] * 12,
        out_specs=(vm, vm),
        scratch_shapes=[
            pltpu.VMEM((2, width, qkv), BF16),
            pltpu.VMEM((2, inner, width), BF16),
            pltpu.VMEM((2,) + kv_cache.shape[1:], BF16),
            pltpu.VMEM(head_weight.shape, BF16),
            pltpu.VMEM((rows, width), BF16),
            pltpu.VMEM((rows, width), BF16),
            pltpu.VMEM((rows, width), BF16),
            pltpu.VMEM((rows * group, HEAD_DIM), F32),
            pltpu.VMEM((2, phases, n, span, HEAD_DIM), BF16),
            pltpu.VMEM((2, phases, n, span, HEAD_DIM), BF16),
            pltpu.VMEM((2, 8, 128), F32),
            pltpu.VMEM((2, n, 8, 128), F32),
            pltpu.VMEM((2, 1, width), BF16),
            pltpu.VMEM((2, 1, qkv), BF16),
            pltpu.VMEM((width // 128, 128), BF16),
            pltpu.VMEM((1, rows), jnp.int32),
            pltpu.VMEM((1, rows), jnp.int32),
            pltpu.VMEM((1, rows), jnp.int32),
            pltpu.VMEM((1, HEAD_DIM), F32),
            pltpu.SMEM((1, rows), jnp.int32),
            pltpu.VMEM((2, heads_all, HEAD_DIM), F32),
            pltpu.VMEM((span, HEAD_DIM), F32),
            pltpu.VMEM((span, HEAD_DIM), F32),
            pltpu.VMEM((span, HEAD_DIM), F32),
            pltpu.VMEM((rows, 128), F32),
            pltpu.VMEM((span, HEAD_DIM), F32),
            pltpu.VMEM((2, KV_HEADS, span, HEAD_DIM), BF16),
            pltpu.VMEM((2, KV_HEADS, n, span, HEAD_DIM), BF16),
            pltpu.VMEM((rows, width), F32),
            pltpu.VMEM((2, n, chunks, rows // 2, width // chunks), BF16),
            pltpu.VMEM((n, 1, 128), F32),
            pltpu.VMEM((1, 128), F32),
            pltpu.VMEM((total, 1, 128), F32),
            pltpu.VMEM((rows, vocab), F32),
            dma((phases,)),
            dma((3,)),
            dma((9,)),
            dma((2,)),
            dma((2, phases)),
            dma((2,)),
            dma((2,)),
            dma((2,)),
            dma((2, KV_HEADS)),
            dma,
            dma,
            dma,
            dma((n,)),
            dma,
            dma((n,)),
            dma,
            dma,
            dma,
            dma,
            dma((chunks + 1,)),
            dma,
            dma,
            dma,
            dma((5,)),
        ],
        compiler_params=pltpu.CompilerParams(
            collective_id=0, has_side_effects=True, vmem_limit_bytes=60 * 1024 * 1024
        ),
    )(
        hidden_in,
        lengths.reshape(1, rows),
        assign.reshape(1, rows),
        token_ids.reshape(1, rows),
        attn_gain,
        qkv_weight,
        qkv_bias,
        out_weight,
        kv_cache,
        final_gain.reshape(width // 128, 128),
        head_weight,
        freq,
    )
    return logprobs, chosen[0, :rows]


def solution(mesh):
    return jax.shard_map(
        local,
        mesh=mesh,
        in_specs=(
            P(None, "mp"),
            P(),
            P(),
            P(),
            P("pipe", "mp"),
            P("pipe", "mp", None),
            P("pipe", None),
            P("pipe", None, "mp"),
            P("pipe", "mp", None, None, None, None),
            P("mp"),
            P(None, ("pipe", "mp")),
        ),
        out_specs=(P(None, ("pipe", "mp")), P()),
        check_vma=False,
    )
```

```python
import functools

import jax
import jax.numpy as jnp
import numpy as np
from jax import lax
from jax.experimental import pallas as pl
from jax.experimental.pallas import tpu as pltpu
from jax.sharding import PartitionSpec as P

HEADS = 32
KV_HEADS = 4
HEAD_DIM = 128
EPS = 1e-06
THETA = 1000000.0
MESH = pl.DeviceIdType.MESH
F32 = jnp.float32
BF16 = jnp.bfloat16


def remote(src, dst, send_sem, recv_sem, device):
    return pltpu.make_async_remote_copy(
        src_ref=src,
        dst_ref=dst,
        send_sem=send_sem,
        recv_sem=recv_sem,
        device_id=device,
        device_id_type=MESH,
    )


def kernel(
    sections,
    n,
    hidden,
    lengths,
    assign,
    token_ids,
    gain,
    qkv_weight,
    bias,
    out_weight,
    cache,
    final_gain,
    head_weight,
    freq,
    out,
    chosen,
    wq,
    wo,
    kv,
    hw,
    x,
    xo,
    scaled,
    stage,
    part,
    part_in,
    sq,
    sq_in,
    gain_v,
    bias_v,
    final_v,
    len_v,
    slot_v,
    token_v,
    freq_v,
    slot_s,
    bias_rows,
    turn_cos,
    turn_sin,
    own_rows,
    target_v,
    fresh,
    att,
    att_in,
    update,
    fin,
    fsq_in,
    red,
    red_in,
    flat,
    wq_sem,
    w_sem,
    small_sem,
    part_s,
    part_r,
    sq_s,
    sq_r,
    att_s,
    att_r,
    hop_s,
    hop_r,
    fin_s,
    fin_r,
    sib_s,
    sib_r,
    fsq_s,
    fsq_r,
    fp_s,
    fq_s,
    fp_r,
    red_s,
    red_r,
    help_s,
    help_r,
    side_s,
):
    sec = lax.axis_index("pipe")
    me = lax.axis_index("mp")
    total = sections * n
    rows, width = x.shape
    lc = kv.shape[1]
    heads_all = HEADS + 2 * KV_HEADS
    group = HEADS // KV_HEADS
    phases = heads_all // group
    span = lc * group
    last = sections - 1
    scale = HEAD_DIM ** (-0.5)
    cw = group * HEAD_DIM
    half = rows // 2
    chunks = fin.shape[2]
    chunk = width // chunks
    parts = 2
    cut = width // parts
    core = lax.rem(sec, 2)
    sibling = sec + 1 - 2 * core
    mine = sec * n + me
    runs = (sec < 2) | (core == 1)
    helps = (sec >= 2) & (core == 0)
    helped = (sec >= 2) & (core == 1)
    following = jnp.where(sec == 0, 1, sec + 2)
    early = min(2, phases)

    def mate(own, k, count):
        if count & (count - 1):
            return lax.rem(own + k, count), lax.rem(own + count - k, count)
        other = 0
        for b in range(count.bit_length() - 1):
            place = 1 << b
            mine_bit = lax.rem(own // place, 2)
            if isinstance(k, int):
                bit = 1 - mine_bit if (k // place) % 2 else mine_bit
            else:
                flip = lax.rem(k // place, 2)
                bit = mine_bit + flip - 2 * mine_bit * flip
            other = other + place * bit
        return other, other

    pairs = [mate(me, k, n) for k in range(n)]
    far_first = range(n - 1, 0, -1)

    def to_peer(k):
        return pairs[k][0]

    def from_peer(k):
        return pairs[k][1]

    def wq_copy(c):
        cols = pl.ds(pl.multiple_of(c * cw, cw), cw)
        return pltpu.make_async_copy(qkv_weight.at[0, :, cols], wq.at[1, :, cols], wq_sem.at[c])

    def phase_of(k):
        return lax.rem(k + phases - 1, phases)

    def small(i, src, dst):
        return pltpu.make_async_copy(src, dst, small_sem.at[i])

    hidden_copy = small(0, hidden, x)
    gain_copy = small(1, gain, gain_v.at[1])
    others = [
        small(2, bias, bias_v.at[1]),
        small(3, final_gain, final_v),
        small(4, lengths, len_v),
        small(5, assign, slot_v),
        small(6, token_ids, token_v),
        small(7, freq, freq_v),
        small(8, assign, slot_s),
    ]

    @pl.when(sec == 0)
    def _():
        hidden_copy.start()

    @pl.when(runs)
    def _():
        gain_copy.start()
        for k in range(early):
            wq_copy((k + phases - 1) % phases).start()

    def wq_rest():
        for k in range(early, phases):
            wq_copy((k + phases - 1) % phases).start()

    kv_copy = pltpu.make_async_copy(cache.at[0], kv.at[1], w_sem.at[0])
    wo_copy = pltpu.make_async_copy(out_weight.at[0], wo.at[1], w_sem.at[1])
    hw_copy = pltpu.make_async_copy(head_weight, hw, w_sem.at[2])

    barrier = pltpu.get_barrier_semaphore()
    for k in far_first:
        pl.semaphore_signal(barrier, inc=1, device_id=(sec, to_peer(k)), device_id_type=MESH)
    for k in range(1, sections):
        pl.semaphore_signal(
            barrier, inc=1, device_id=(lax.rem(sec + k, sections), me), device_id_type=MESH
        )
    @pl.when(sec > 0)
    def _():
        for copy in others:
            copy.start()
        hw_copy.start()

    @pl.when((sec > 0) & runs)
    def _():
        wq_rest()
        kv_copy.start()
        wo_copy.start()

    def help_copy(i, src, dst):
        return remote(src, dst, help_s, help_r.at[i], (sibling, me))

    help_copies = [
        help_copy(0, gain, gain_v.at[0]),
        help_copy(1, bias, bias_v.at[0]),
        help_copy(2, qkv_weight.at[0], wq.at[0]),
        help_copy(3, cache.at[0], kv.at[0]),
        help_copy(4, out_weight.at[0], wo.at[0]),
    ]

    eye = lax.broadcasted_iota(jnp.int32, (rows, 128), 0) == lax.broadcasted_iota(
        jnp.int32, (rows, 128), 1
    )

    def to_row(col):
        return jnp.sum(jnp.where(eye, col, 0.0), axis=0, keepdims=True)

    def to_col(row):
        return jnp.sum(jnp.where(eye, row, 0.0), axis=1, keepdims=True)

    lane = lax.broadcasted_iota(jnp.int32, (1, HEAD_DIM), 1)
    lane_rows = lax.broadcasted_iota(jnp.int32, (1, rows), 1)
    small_eye = lax.broadcasted_iota(jnp.int32, (rows, rows), 0) == lax.broadcasted_iota(
        jnp.int32, (rows, rows), 1
    )

    def set_bias(t):
        for i in range(heads_all):
            bias_rows[t, i : i + 1, :] = bias_v[
                t, :, i * HEAD_DIM : (i + 1) * HEAD_DIM
            ].astype(F32)

    def set_up():
        for copy in others:
            copy.wait()
        set_bias(1)
        target = jnp.sum(
            jnp.where(small_eye, token_v[...].astype(F32), 0.0), axis=1, keepdims=True
        )
        target_v[...] = jnp.broadcast_to(target, target_v.shape)
        length = jnp.concatenate(
            [
                jnp.sum(
                    jnp.where(lane_rows == me * lc + i, len_v[...].astype(F32), 0.0),
                    axis=1,
                    keepdims=True,
                )
                for i in range(lc)
            ],
            axis=0,
        )
        angles = length * freq_v[...]
        cosines = jnp.cos(angles)
        sines = jnp.sin(angles) * jnp.where(lane < HEAD_DIM // 2, -1.0, 1.0)
        for i in range(lc):
            own = slice(i * group, (i + 1) * group)
            own_rows[own, :] = jnp.broadcast_to(length[i : i + 1], (group, HEAD_DIM))
            turn_cos[own, :] = jnp.broadcast_to(cosines[i : i + 1], (group, HEAD_DIM))
            turn_sin[own, :] = jnp.broadcast_to(sines[i : i + 1], (group, HEAD_DIM))

    def scale_rows(t):
        current = x[...].astype(F32)
        sq[t] = jnp.broadcast_to(
            to_row(jnp.sum(current * current, axis=1, keepdims=True)), sq.shape[1:]
        )
        scaled[...] = (current * gain_v[t].astype(F32)).astype(BF16)

    def sq_copy(t, peer, slot):
        return remote(sq.at[t], sq_in.at[t, slot], sq_s.at[t], sq_r.at[t], (sec, peer))

    def sq_send(t):
        for k in far_first:
            sq_copy(t, to_peer(k), me).start()
        sq_in[t, me] = sq[t]

    def part_copy(t, phase, peer, slot):
        return remote(
            part.at[t, phase, peer],
            part_in.at[t, phase, slot],
            part_s.at[t],
            part_r.at[t, phase],
            (sec, peer),
        )

    def multiply(t, phase):
        if t == 1:
            wq_copy(phase).wait()
        base = pl.multiple_of(phase * cw, cw)
        piece = jnp.dot(scaled[...], wq[t, :, pl.ds(base, cw)], preferred_element_type=F32)
        for j in range(group):
            stage[pl.ds(j, rows, stride=group), :] = piece[
                :, j * HEAD_DIM : (j + 1) * HEAD_DIM
            ]
        for p in range(n):
            part[t, phase, p] = stage[p * span : (p + 1) * span, :].astype(BF16)

    def spread(t, phase):
        for k in far_first:
            part_copy(t, phase, to_peer(k), me).start()
        part_in[t, phase, me] = part[t, phase, me]

    def compute_only(k, carry):
        multiply(1, phase_of(k))
        return carry

    def send_only(k, carry):
        spread(1, phase_of(k))
        return carry

    def project(t):
        def one(k, carry):
            multiply(t, phase_of(k))
            spread(t, phase_of(k))
            return carry

        return one

    def hop_copy(c, to):
        cols = pl.ds(c * cut, cut)
        return remote(xo.at[:, cols], x.at[:, cols], hop_s, hop_r, (to, me))


    @pl.when(sec == 0)
    def _():
        with jax.named_scope("hidden_wait"):
            hidden_copy.wait()
        gain_copy.wait()
        scale_rows(1)
        wq_rest()
        for copy in others:
            copy.start()
        lax.fori_loop(0, early, compute_only, 0)

    @pl.when(sec > 0)
    def _():
        set_up()

    with jax.named_scope("barrier"):
        pl.semaphore_wait(barrier, n + sections - 2)

    @pl.when(helps)
    def _():
        for copy in help_copies:
            copy.start()

    pos = lax.broadcasted_iota(jnp.int32, (1, kv.shape[4]), 1).astype(F32)
    own_request = me * lc + lax.broadcasted_iota(jnp.int32, (span, 128), 0) // group
    own_lane = lax.broadcasted_iota(jnp.int32, (span, 128), 1)
    is_key = (
        lax.rem(lax.broadcasted_iota(jnp.int32, (span, HEAD_DIM), 0), 2 * KV_HEADS) < KV_HEADS
    )

    def turned(block):
        return block * turn_cos[...] + pltpu.roll(block, HEAD_DIM // 2, 1) * turn_sin[...]

    def each(rows_of):
        return jnp.concatenate([rows_of(i) for i in range(lc)], axis=0)

    def rows_at(i):
        return slice(i * group, (i + 1) * group)

    def att_copy(t, h, peer, slot):
        return remote(
            att.at[t, h], att_in.at[t, h, slot], att_s.at[t], att_r.at[t, h], (sec, peer)
        )

    def all_att(t, h):
        return remote(
            att_in.at[t, h, pl.ds(1, n - 1)],
            att_in.at[t, h, pl.ds(1, n - 1)],
            att_s.at[t],
            att_r.at[t, h],
            (sec, me),
        )

    def summed(t, phase):
        with jax.named_scope("rs_wait"):
            remote(
                part.at[t, phase, pl.ds(1, n - 1)],
                part_in.at[t, phase, pl.ds(1, n - 1)],
                part_s.at[t],
                part_r.at[t, phase],
                (sec, me),
            ).wait_recv()
        result = part_in[t, phase, 0].astype(F32)
        for p in range(1, n):
            result = result + part_in[t, phase, p].astype(F32)
        return result

    def attention(t):
        with jax.named_scope("sq_wait"):
            remote(
                sq_in.at[t, pl.ds(1, n - 1)],
                sq_in.at[t, pl.ds(1, n - 1)],
                sq_s.at[t],
                sq_r.at[t],
                (sec, me),
            ).wait_recv()
        squares = sq_in[t, 0]
        for p in range(1, n):
            squares = squares + sq_in[t, p]
        factor = lax.rsqrt(
            jnp.sum(
                jnp.where(own_lane == own_request, squares[0:1, :], 0.0), axis=1, keepdims=True
            )
            / (n * width)
            + EPS
        )
        fresh_bias = bias_rows[t, HEADS:, :]
        block = summed(t, phases - 1) * factor + each(lambda i: fresh_bias)
        fresh[...] = jnp.where(is_key, turned(block), block).astype(BF16).astype(F32)
        if t == 1:
            kv_copy.wait()
        else:
            help_copies[3].wait_recv()

        def attend(h, carry):
            block_sum = summed(t, h)
            with jax.named_scope("attend"):
                bias_h = bias_rows[t, pl.ds(pl.multiple_of(h * group, group), group), :]
                query = turned(block_sum * factor + each(lambda i: bias_h))
                scores = each(
                    lambda i: lax.dot_general(
                        query[rows_at(i)].astype(BF16),
                        kv[t, i, 0, h],
                        (((1,), (1,)), ((), ())),
                        preferred_element_type=F32,
                    )
                )
                scores = scores * scale
                repeat = lambda row: jnp.broadcast_to(
                    fresh[pl.ds(row, 1), :], (group, HEAD_DIM)
                )
                key_new = each(lambda i: repeat(i * group + h))
                value_new = each(lambda i: repeat(i * group + KV_HEADS + h))
                self_score = (
                    jnp.sum(query.astype(BF16).astype(F32) * key_new, axis=1, keepdims=True)
                    * scale
                )
                visible = pos < own_rows[:, 0:1]
                top = jnp.maximum(
                    jnp.max(jnp.where(visible, scores, -1e30), axis=1, keepdims=True),
                    self_score,
                )
                weights = jnp.where(visible, jnp.exp(scores - top), 0.0)
                self_weight = jnp.exp(self_score - top)
                denominator = jnp.sum(weights, axis=1, keepdims=True) + self_weight
                mixed = each(
                    lambda i: jnp.dot(
                        weights[rows_at(i)].astype(BF16),
                        kv[t, i, 1, h],
                        preferred_element_type=F32,
                    )
                )
                mixed = mixed + self_weight.astype(BF16).astype(F32) * value_new
                att[t, h] = (mixed / denominator).astype(BF16)
            for k in far_first:
                att_copy(t, h, to_peer(k), me).start()
            att_in[t, h, me] = att[t, h]
            return carry

        lax.fori_loop(0, KV_HEADS, attend, 0)
        if t == 1:
            wo_copy.wait()
        else:
            help_copies[4].wait_recv()
        update[...] = x[...].astype(F32)

        def project_out(h, carry):
            mat = gathered(t, h)
            depth = pl.ds(pl.multiple_of(h * cw, cw), cw)
            update[...] += jnp.dot(mat, wo[t, depth, :], preferred_element_type=F32)
            return carry

        lax.fori_loop(0, KV_HEADS - 1, project_out, 0)

    def gathered(t, h):
        with jax.named_scope("ag_wait"):
            all_att(t, h).wait_recv()
        for p in range(n):
            stage[p * span : (p + 1) * span, :] = att_in[t, h, p].astype(F32)
        return jnp.concatenate(
            [stage[pl.ds(j, rows, stride=group), :].astype(BF16) for j in range(group)],
            axis=1,
        )

    top_rows = (KV_HEADS - 1) * cw

    def grown(t, mat, cols):
        return (
            update[:, cols]
            + jnp.dot(
                mat, wo[t, top_rows : top_rows + cw, cols], preferred_element_type=F32
            )
        ).astype(BF16)

    @pl.when(sec == 0)
    def _():
        sq_send(1)
        lax.fori_loop(0, early, send_only, 0)

    @pl.when(core == 1)
    def _():
        gain_copy.wait()
        with jax.named_scope("hop_wait"):
            remote(xo, x, hop_s, hop_r, (sec - 1, me)).wait_recv()

    @pl.when(helped)
    def _():
        help_copies[0].wait_recv()
        help_copies[1].wait_recv()
        help_copies[2].wait_recv()
        scale_rows(0)
        sq_send(0)
        lax.fori_loop(0, phases, project(0), 0)
        set_bias(0)
        attention(0)
        x[...] = grown(0, gathered(0, KV_HEADS - 1), slice(0, width))

    @pl.when(core == 1)
    def _():
        scale_rows(1)
        sq_send(1)

    @pl.when(runs)
    def _():
        lax.fori_loop(jnp.where(sec == 0, early, 0), phases, project(1), 0)

    @pl.when(sec == 0)
    def _():
        kv_copy.start()
        wo_copy.start()
        hw_copy.start()
        set_up()

    def fin_copy(c, peer, slot):
        return remote(
            fin.at[core, slot, c],
            fin.at[core, slot, c],
            fin_s,
            fin_r.at[slot],
            (sec, peer),
        )

    def sib_copy(c, piece, slot):
        return remote(
            fin.at[piece, slot, c],
            fin.at[piece, slot, c],
            sib_s,
            sib_r.at[slot],
            (sibling, me),
        )

    def fsq_copy(peer, slot):
        return remote(
            fsq_in.at[slot], fsq_in.at[slot], fsq_s, fsq_r, (sec, peer)
        )

    across = max(d for d in range(1, n + 1) if n % d == 0 and d * d <= n)
    relayed = across == 2 and n == 8
    place = me // across
    outer = (place == 0) | (place == n // across - 1)

    def fin_send():
        for k in (1, 6, 4, 5, 7, 2, 3) if relayed else range(1, n):
            if relayed and k in (5, 7):

                @pl.when(jnp.logical_not(outer))
                def _():
                    fin_copy(0, to_peer(k), me).start()

            else:
                fin_copy(0, to_peer(k), me).start()

    def side_copy(slot):
        return remote(
            fin.at[core, slot], fin.at[core, slot], side_s, fin_r.at[slot], (sec, to_peer(1))
        )

    def fp_copy(c, k):
        to = lax.rem(sec + k, sections)
        piece = lax.rem(to, 2)
        return remote(
            fin.at[piece, me, c], fin.at[piece, me, c], fp_s, fp_r.at[c], (to, me)
        )

    def fp_sq(k):
        to = lax.rem(sec + k, sections)
        return remote(
            fsq_in.at[me], fsq_in.at[me], fq_s, fp_r.at[chunks], (to, me)
        )

    @pl.when(runs)
    def _():
        attention(1)
        mat = gathered(1, KV_HEADS - 1)
        final_sq = jnp.zeros((rows, 1), F32)
        for c in range(parts):
            cols = slice(c * cut, (c + 1) * cut)
            new = grown(1, mat, cols)
            xo[:, cols] = new
            final = new.astype(F32)
            final_sq = final_sq + jnp.sum(final * final, axis=1, keepdims=True)

            @pl.when(sec < last)
            def _():
                hop_copy(c, following).start()

            @pl.when(sec == last)
            def _():
                lanes = cut // 128
                row = jnp.concatenate(
                    [
                        final_v[c * lanes + i : c * lanes + i + 1, :].astype(F32)
                        for i in range(lanes)
                    ],
                    axis=1,
                )
                both = (final * row).astype(BF16)
                fin[0, me, 0, :, cols] = both[:half]
                fin[1, me, 0, :, cols] = both[half:]

        @pl.when(sec == last)
        def _():
            for k in range(1, sections):
                fp_copy(0, k).start()
            fin_send()
            sib_copy(0, core, me).start()
            fsq_in[me] = to_row(final_sq)
            for k in range(1, sections):
                fp_sq(k).start()
            for k in far_first:
                fsq_copy(to_peer(k), me).start()

    @pl.when(sec < last)
    def _():
        for c in range(chunks):
            arriving = remote(
                fin.at[core, me, c], fin.at[core, me, c], fp_s, fp_r.at[c], (last, me)
            )
            with jax.named_scope("fp_wait"):
                arriving.wait_recv()
            fin_send()

            @pl.when(sec < last - 1)
            def _():
                sib_copy(c, core, me).start()

        arriving = remote(
            fsq_in.at[me], fsq_in.at[me], fq_s, fp_r.at[chunks], (last, me)
        )
        arriving.wait_recv()
        for k in far_first:
            fsq_copy(to_peer(k), me).start()

    hw_copy.wait()

    def whole(piece, slot, send, recv):
        return remote(fin.at[piece, slot], fin.at[piece, slot], send, recv.at[slot], (sibling, me))

    far = jnp.where(outer, 6, 4)
    arrivals = [0, 1, far, 2, 3, 10 - far, 11 - far, far + 1]

    def arriving_from(k):
        return mate(me, arrivals[k] if relayed else k, n)[1]

    def pass_on(k):
        peer = arriving_from(k)
        with jax.named_scope("fin_wait"):
            whole(core, peer, fin_s, fin_r).wait_recv()
        if relayed and k == 2:
            side_copy(peer).start()

        for c in range(chunks):
            sib_copy(c, core, peer).start()

    def head(k, logits):
        peer = arriving_from(k)
        if isinstance(k, int) and k == 0:

            @pl.when(sec < last)
            def _():
                whole(1 - core, peer, sib_s, sib_r).wait_recv()

        else:
            with jax.named_scope("sib_wait"):
                whole(1 - core, peer, sib_s, sib_r).wait_recv()
        for c in range(chunks):
            at = pl.ds(pl.multiple_of(peer * width + c * chunk, chunk), chunk)
            both = jnp.concatenate([fin[0, peer, c], fin[1, peer, c]], axis=0)
            logits = logits + jnp.dot(both, hw[at, :], preferred_element_type=F32)
        return logits

    lag = min(2, n - 1)
    for k in range(1, lag + 1):
        pass_on(k)
    logits = head(0, jnp.zeros(out.shape, F32))

    def step(k, logits):
        pass_on(k)
        return head(k - lag, logits)

    if relayed:
        for k in range(lag + 1, n):
            logits = step(k, logits)
        for k in range(n - lag, n):
            logits = head(k, logits)
    else:
        logits = lax.fori_loop(lag + 1, n, step, logits)
        logits = lax.fori_loop(n - lag, n, head, logits)
    all_fsq = remote(
        fsq_in.at[pl.ds(1, n - 1)], fsq_in.at[pl.ds(1, n - 1)], fsq_s, fsq_r, (sec, me)
    )
    all_fsq.wait_recv()
    squares = jnp.sum(fsq_in[:, 0, :], axis=0, keepdims=True)
    logits = logits * lax.rsqrt(to_col(squares) / (n * width) + EPS)
    vocab = out.shape[1]
    ids = (mine * vocab + lax.broadcasted_iota(jnp.int32, (1, vocab), 1)).astype(F32)
    picked = jnp.sum(jnp.where(ids == target_v[:, 0:1], logits, 0.0), axis=1, keepdims=True)
    top = jnp.max(logits, axis=1, keepdims=True)
    amount = jnp.sum(jnp.exp(logits - top), axis=1, keepdims=True)
    row_of = lax.broadcasted_iota(jnp.int32, (rows, 128), 0)
    lane_of = lax.broadcasted_iota(jnp.int32, (rows, 128), 1)
    packed = jnp.where(lane_of == row_of, top, 0.0)
    packed = jnp.where(lane_of == row_of + rows, amount, packed)
    packed = jnp.where(lane_of == row_of + 2 * rows, picked, packed)
    red[...] = jnp.sum(packed, axis=0, keepdims=True)

    def red_copy(other, slot):
        return remote(
            red, red_in.at[slot], red_s, red_r, (other // n, lax.rem(other, n))
        )

    if total <= 64:
        for k in range(total - 1, 0, -1):
            red_copy(mate(mine, k, total)[0], mine).start()
    else:

        def red_start(k, carry):
            red_copy(mate(mine, total - k, total)[0], mine).start()
            return carry

        lax.fori_loop(1, total, red_start, 0)
    red_in[mine] = red[...]
    flat[...] = logits

    def sent(ref, sem):
        remote(ref, ref, sem, sem, (sec, me)).wait_send()

    others_n = pl.ds(1, n - 1)

    def stage_sent(t):
        sent(sq_in.at[t, others_n], sq_s.at[t])
        sent(part_in.at[t, :, others_n], part_s.at[t])
        sent(att_in.at[t, :, others_n], att_s.at[t])

    @pl.when(helped)
    def _():
        stage_sent(0)

    @pl.when(runs)
    def _():
        stage_sent(1)

    @pl.when(helps)
    def _():
        for copy in help_copies:
            copy.wait_send()

    if relayed:
        sent(fin.at[0, pl.ds(0, n - 3)], fin_s)
        sent(fin.at[0, 0], side_s)

        @pl.when(jnp.logical_not(outer))
        def _():
            sent(fin.at[0, pl.ds(0, 2)], fin_s)

    else:
        sent(fin.at[0, others_n], fin_s)
    sent(fin.at[0, others_n], sib_s)
    all_fsq.wait_send()

    @pl.when(sec != last - 1)
    def _():
        sent(fin.at[0, 0], sib_s)

    @pl.when((sec < last) & runs)
    def _():
        sent(xo, hop_s)

    @pl.when(sec == last)
    def _():
        sent(fin.at[0, pl.ds(1, sections - 1)], fp_s)
        sent(fsq_in.at[pl.ds(1, sections - 1)], fq_s)

    order = (
        jnp.sum(jnp.where(small_eye, slot_v[...].astype(F32), 0.0), axis=1, keepdims=True)
        == lane_of.astype(F32)
    )
    for s in range(rows):
        out[s : s + 1, :] = flat[pl.ds(slot_s[0, s], 1), :]

    everyone = remote(
        red_in.at[pl.ds(1, total - 1)],
        red_in.at[pl.ds(1, total - 1)],
        red_s,
        red_r,
        (sec, me),
    )
    with jax.named_scope("red_wait"):
        everyone.wait_recv()
    seen = red_in[:, 0, :]
    row_top = jnp.max(seen, axis=0, keepdims=True)
    amounts = pltpu.roll(seen, 128 - rows, 1)
    row_total = jnp.sum(amounts * jnp.exp(jnp.minimum(seen - row_top, 0.0)), axis=0, keepdims=True)
    log_total = row_top + jnp.log(row_total)
    total_col = jnp.sum(jnp.where(order, log_total, 0.0), axis=1, keepdims=True)
    out[...] = out[...] - total_col
    scored = pltpu.roll(jnp.sum(seen, axis=0, keepdims=True), 128 - 2 * rows, 1) - log_total
    chosen[...] = to_row(jnp.sum(jnp.where(order, scored, 0.0), axis=1, keepdims=True))
    with jax.named_scope("red_sent"):
        everyone.wait_send()


def local(
    hidden_in,
    lengths,
    assign,
    token_ids,
    attn_gain,
    qkv_weight,
    qkv_bias,
    out_weight,
    kv_cache,
    final_gain,
    head_weight,
):
    sections = lax.axis_size("pipe")
    n = lax.axis_size("mp")
    rows, width = hidden_in.shape
    lc = kv_cache.shape[1]
    qkv = qkv_weight.shape[2]
    inner = out_weight.shape[1]
    vocab = head_weight.shape[1]
    heads_all = HEADS + 2 * KV_HEADS
    half = HEAD_DIM // 2
    frequency = np.float32(THETA) ** (
        -np.arange(half).astype(np.float32) * np.float32(2.0) / np.float32(HEAD_DIM)
    )
    freq = jnp.asarray(np.concatenate([frequency, frequency])[None, :], F32)
    group = HEADS // KV_HEADS
    phases = heads_all // group
    span = lc * group
    dma = pltpu.SemaphoreType.DMA
    vm = pl.BlockSpec(memory_space=pltpu.VMEM)
    hbm = pl.BlockSpec(memory_space=pltpu.HBM)
    total = sections * n
    chunks = 1
    logprobs, chosen = pl.pallas_call(
        functools.partial(kernel, sections, n),
        out_shape=(
            pltpu.VMEM((rows, vocab), F32),
            pltpu.VMEM((1, 128), F32),
        ),
        in_specs=[hbm] * 12,
        out_specs=(vm, vm),
        scratch_shapes=[
            pltpu.VMEM((2, width, qkv), BF16),
            pltpu.VMEM((2, inner, width), BF16),
            pltpu.VMEM((2,) + kv_cache.shape[1:], BF16),
            pltpu.VMEM(head_weight.shape, BF16),
            pltpu.VMEM((rows, width), BF16),
            pltpu.VMEM((rows, width), BF16),
            pltpu.VMEM((rows, width), BF16),
            pltpu.VMEM((rows * group, HEAD_DIM), F32),
            pltpu.VMEM((2, phases, n, span, HEAD_DIM), BF16),
            pltpu.VMEM((2, phases, n, span, HEAD_DIM), BF16),
            pltpu.VMEM((2, 8, 128), F32),
            pltpu.VMEM((2, n, 8, 128), F32),
            pltpu.VMEM((2, 1, width), BF16),
            pltpu.VMEM((2, 1, qkv), BF16),
            pltpu.VMEM((width // 128, 128), BF16),
            pltpu.VMEM((1, rows), jnp.int32),
            pltpu.VMEM((1, rows), jnp.int32),
            pltpu.VMEM((1, rows), jnp.int32),
            pltpu.VMEM((1, HEAD_DIM), F32),
            pltpu.SMEM((1, rows), jnp.int32),
            pltpu.VMEM((2, heads_all, HEAD_DIM), F32),
            pltpu.VMEM((span, HEAD_DIM), F32),
            pltpu.VMEM((span, HEAD_DIM), F32),
            pltpu.VMEM((span, HEAD_DIM), F32),
            pltpu.VMEM((rows, 128), F32),
            pltpu.VMEM((span, HEAD_DIM), F32),
            pltpu.VMEM((2, KV_HEADS, span, HEAD_DIM), BF16),
            pltpu.VMEM((2, KV_HEADS, n, span, HEAD_DIM), BF16),
            pltpu.VMEM((rows, width), F32),
            pltpu.VMEM((2, n, chunks, rows // 2, width // chunks), BF16),
            pltpu.VMEM((n, 1, 128), F32),
            pltpu.VMEM((1, 128), F32),
            pltpu.VMEM((total, 1, 128), F32),
            pltpu.VMEM((rows, vocab), F32),
            dma((phases,)),
            dma((3,)),
            dma((9,)),
            dma((2,)),
            dma((2, phases)),
            dma((2,)),
            dma((2,)),
            dma((2,)),
            dma((2, KV_HEADS)),
            dma,
            dma,
            dma,
            dma((n,)),
            dma,
            dma((n,)),
            dma,
            dma,
            dma,
            dma,
            dma((chunks + 1,)),
            dma,
            dma,
            dma,
            dma((5,)),
            dma,
        ],
        compiler_params=pltpu.CompilerParams(
            collective_id=0, has_side_effects=True, vmem_limit_bytes=60 * 1024 * 1024
        ),
    )(
        hidden_in,
        lengths.reshape(1, rows),
        assign.reshape(1, rows),
        token_ids.reshape(1, rows),
        attn_gain,
        qkv_weight,
        qkv_bias,
        out_weight,
        kv_cache,
        final_gain.reshape(width // 128, 128),
        head_weight,
        freq,
    )
    return logprobs, chosen[0, :rows]


def solution(mesh):
    return jax.shard_map(
        local,
        mesh=mesh,
        in_specs=(
            P(None, "mp"),
            P(),
            P(),
            P(),
            P("pipe", "mp"),
            P("pipe", "mp", None),
            P("pipe", None),
            P("pipe", None, "mp"),
            P("pipe", "mp", None, None, None, None),
            P("mp"),
            P(None, ("pipe", "mp")),
        ),
        out_specs=(P(None, ("pipe", "mp")), P()),
        check_vma=False,
    )
```

```python
import functools

import jax
import jax.numpy as jnp
import numpy as np
from jax import lax
from jax.experimental import pallas as pl
from jax.experimental.pallas import tpu as pltpu
from jax.sharding import PartitionSpec as P

HEADS = 32
KV_HEADS = 4
HEAD_DIM = 128
EPS = 1e-06
THETA = 1000000.0
MESH = pl.DeviceIdType.MESH
F32 = jnp.float32
BF16 = jnp.bfloat16


def remote(src, dst, send_sem, recv_sem, device):
    return pltpu.make_async_remote_copy(
        src_ref=src,
        dst_ref=dst,
        send_sem=send_sem,
        recv_sem=recv_sem,
        device_id=device,
        device_id_type=MESH,
    )


def kernel(
    sections,
    n,
    hidden,
    lengths,
    assign,
    token_ids,
    gain,
    qkv_weight,
    bias,
    out_weight,
    cache,
    final_gain,
    head_weight,
    freq,
    out,
    chosen,
    wq,
    wo,
    kv,
    hw,
    x,
    xo,
    scaled,
    stage,
    part,
    part_in,
    sq,
    sq_in,
    gain_v,
    bias_v,
    final_v,
    len_v,
    slot_v,
    token_v,
    freq_v,
    slot_s,
    bias_rows,
    turn_cos,
    turn_sin,
    own_rows,
    target_v,
    fresh,
    att,
    att_in,
    update,
    fin,
    fsq_in,
    red,
    red_in,
    flat,
    wq_sem,
    w_sem,
    small_sem,
    part_s,
    part_r,
    sq_s,
    sq_r,
    att_s,
    att_r,
    hop_s,
    hop_r,
    fin_s,
    fin_r,
    sib_s,
    sib_r,
    fsq_s,
    fsq_r,
    fp_s,
    fq_s,
    fp_r,
    red_s,
    red_r,
    help_s,
    help_r,
    side_s,
):
    sec = lax.axis_index("pipe")
    me = lax.axis_index("mp")
    total = sections * n
    rows, width = x.shape
    lc = kv.shape[1]
    heads_all = HEADS + 2 * KV_HEADS
    group = HEADS // KV_HEADS
    phases = heads_all // group
    span = lc * group
    last = sections - 1
    scale = HEAD_DIM ** (-0.5)
    cw = group * HEAD_DIM
    half = rows // 2
    chunks = fin.shape[2]
    chunk = width // chunks
    parts = 2
    cut = width // parts
    core = lax.rem(sec, 2)
    sibling = sec + 1 - 2 * core
    mine = sec * n + me
    runs = (sec < 2) | (core == 1)
    helps = (sec >= 2) & (core == 0)
    helped = (sec >= 2) & (core == 1)
    following = jnp.where(sec == 0, 1, sec + 2)
    early = min(1, phases)

    def mate(own, k, count):
        if count & (count - 1):
            return lax.rem(own + k, count), lax.rem(own + count - k, count)
        other = 0
        for b in range(count.bit_length() - 1):
            place = 1 << b
            mine_bit = lax.rem(own // place, 2)
            if isinstance(k, int):
                bit = 1 - mine_bit if (k // place) % 2 else mine_bit
            else:
                flip = lax.rem(k // place, 2)
                bit = mine_bit + flip - 2 * mine_bit * flip
            other = other + place * bit
        return other, other

    pairs = [mate(me, k, n) for k in range(n)]
    across = max(d for d in range(1, n + 1) if n % d == 0 and d * d <= n)
    relayed = across == 2 and n == 8
    place = me // across
    outer = (place == 0) | (place == n // across - 1)
    far = jnp.where(outer, 6, 4)
    if relayed:
        far_peers = [
            mate(me, k, n)[0] for k in (far + 1, far, 11 - far, 10 - far, 3, 2, 1)
        ]
    else:
        far_peers = [pairs[k][0] for k in range(n - 1, 0, -1)]

    def to_peer(k):
        return pairs[k][0]

    def from_peer(k):
        return pairs[k][1]

    def wq_copy(c):
        cols = pl.ds(pl.multiple_of(c * cw, cw), cw)
        return pltpu.make_async_copy(qkv_weight.at[0, :, cols], wq.at[1, :, cols], wq_sem.at[c])

    def phase_of(k):
        return lax.rem(k + phases - 1, phases)

    def small(i, src, dst):
        return pltpu.make_async_copy(src, dst, small_sem.at[i])

    hidden_copy = small(0, hidden, x)
    gain_copy = small(1, gain, gain_v.at[1])
    others = [
        small(2, bias, bias_v.at[1]),
        small(3, final_gain, final_v),
        small(4, lengths, len_v),
        small(5, assign, slot_v),
        small(6, token_ids, token_v),
        small(7, freq, freq_v),
        small(8, assign, slot_s),
    ]

    @pl.when(sec == 0)
    def _():
        hidden_copy.start()

    @pl.when(runs)
    def _():
        gain_copy.start()
        for k in range(early):
            wq_copy((k + phases - 1) % phases).start()

    def wq_rest():
        for k in range(early, phases):
            wq_copy((k + phases - 1) % phases).start()

    kv_copy = pltpu.make_async_copy(cache.at[0], kv.at[1], w_sem.at[0])
    wo_copy = pltpu.make_async_copy(out_weight.at[0], wo.at[1], w_sem.at[1])
    hw_copy = pltpu.make_async_copy(head_weight, hw, w_sem.at[2])

    barrier = pltpu.get_barrier_semaphore()
    for peer in far_peers:
        pl.semaphore_signal(barrier, inc=1, device_id=(sec, peer), device_id_type=MESH)
    for k in range(1, sections):
        pl.semaphore_signal(
            barrier, inc=1, device_id=(lax.rem(sec + k, sections), me), device_id_type=MESH
        )
    @pl.when(sec > 0)
    def _():
        for copy in others:
            copy.start()
        hw_copy.start()

    @pl.when((sec > 0) & runs)
    def _():
        wq_rest()
        kv_copy.start()
        wo_copy.start()

    def help_copy(i, src, dst):
        return remote(src, dst, help_s, help_r.at[i], (sibling, me))

    help_copies = [
        help_copy(0, gain, gain_v.at[0]),
        help_copy(1, bias, bias_v.at[0]),
        help_copy(2, qkv_weight.at[0], wq.at[0]),
        help_copy(3, cache.at[0], kv.at[0]),
        help_copy(4, out_weight.at[0], wo.at[0]),
    ]

    eye = lax.broadcasted_iota(jnp.int32, (rows, 128), 0) == lax.broadcasted_iota(
        jnp.int32, (rows, 128), 1
    )

    def to_row(col):
        return jnp.sum(jnp.where(eye, col, 0.0), axis=0, keepdims=True)

    def to_col(row):
        return jnp.sum(jnp.where(eye, row, 0.0), axis=1, keepdims=True)

    lane = lax.broadcasted_iota(jnp.int32, (1, HEAD_DIM), 1)
    lane_rows = lax.broadcasted_iota(jnp.int32, (1, rows), 1)
    small_eye = lax.broadcasted_iota(jnp.int32, (rows, rows), 0) == lax.broadcasted_iota(
        jnp.int32, (rows, rows), 1
    )

    def set_bias(t):
        for i in range(heads_all):
            bias_rows[t, i : i + 1, :] = bias_v[
                t, :, i * HEAD_DIM : (i + 1) * HEAD_DIM
            ].astype(F32)

    def set_up():
        for copy in others:
            copy.wait()
        set_bias(1)
        target = jnp.sum(
            jnp.where(small_eye, token_v[...].astype(F32), 0.0), axis=1, keepdims=True
        )
        target_v[...] = jnp.broadcast_to(target, target_v.shape)
        length = jnp.concatenate(
            [
                jnp.sum(
                    jnp.where(lane_rows == me * lc + i, len_v[...].astype(F32), 0.0),
                    axis=1,
                    keepdims=True,
                )
                for i in range(lc)
            ],
            axis=0,
        )
        angles = length * freq_v[...]
        cosines = jnp.cos(angles)
        sines = jnp.sin(angles) * jnp.where(lane < HEAD_DIM // 2, -1.0, 1.0)
        for i in range(lc):
            own = slice(i * group, (i + 1) * group)
            own_rows[own, :] = jnp.broadcast_to(length[i : i + 1], (group, HEAD_DIM))
            turn_cos[own, :] = jnp.broadcast_to(cosines[i : i + 1], (group, HEAD_DIM))
            turn_sin[own, :] = jnp.broadcast_to(sines[i : i + 1], (group, HEAD_DIM))

    def scale_rows(t):
        current = x[...].astype(F32)
        sq[t] = to_row(jnp.sum(current * current, axis=1, keepdims=True))
        scaled[...] = (current * gain_v[t].astype(F32)).astype(BF16)

    def sq_copy(t, peer, slot):
        return remote(sq.at[t], sq_in.at[t, slot], sq_s.at[t], sq_r.at[t], (sec, peer))

    def sq_send(t):
        for peer in far_peers:
            sq_copy(t, peer, me).start()
        sq_in[t, me] = sq[t]

    def part_copy(t, phase, peer, slot):
        return remote(
            part.at[t, phase, peer],
            part_in.at[t, phase, slot],
            part_s.at[t],
            part_r.at[t, phase],
            (sec, peer),
        )

    def multiply(t, phase):
        if t == 1:
            wq_copy(phase).wait()
        base = pl.multiple_of(phase * cw, cw)
        piece = jnp.dot(scaled[...], wq[t, :, pl.ds(base, cw)], preferred_element_type=F32)
        for j in range(group):
            stage[pl.ds(j, rows, stride=group), :] = piece[
                :, j * HEAD_DIM : (j + 1) * HEAD_DIM
            ]
        for p in range(n):
            part[t, phase, p] = stage[p * span : (p + 1) * span, :].astype(BF16)

    def spread(t, phase):
        for peer in far_peers:
            part_copy(t, phase, peer, me).start()
        part_in[t, phase, me] = part[t, phase, me]

    def compute_only(k, carry):
        multiply(1, phase_of(k))
        return carry

    def send_only(k, carry):
        spread(1, phase_of(k))
        return carry

    def project(t):
        def one(k, carry):
            multiply(t, phase_of(k))
            spread(t, phase_of(k))
            return carry

        return one

    def hop_copy(c, to):
        cols = pl.ds(c * cut, cut)
        return remote(xo.at[:, cols], x.at[:, cols], hop_s, hop_r, (to, me))


    @pl.when(sec == 0)
    def _():
        with jax.named_scope("hidden_wait"):
            hidden_copy.wait()
        gain_copy.wait()
        scale_rows(1)
        wq_rest()
        for copy in others:
            copy.start()
        lax.fori_loop(0, early, compute_only, 0)

    @pl.when(sec > 0)
    def _():
        set_up()

    with jax.named_scope("barrier"):
        pl.semaphore_wait(barrier, n + sections - 2)

    @pl.when(helps)
    def _():
        for copy in help_copies:
            copy.start()

    pos = lax.broadcasted_iota(jnp.int32, (1, kv.shape[4]), 1).astype(F32)
    own_request = me * lc + lax.broadcasted_iota(jnp.int32, (span, 128), 0) // group
    own_lane = lax.broadcasted_iota(jnp.int32, (span, 128), 1)
    is_key = (
        lax.rem(lax.broadcasted_iota(jnp.int32, (span, HEAD_DIM), 0), 2 * KV_HEADS) < KV_HEADS
    )

    def turned(block):
        return block * turn_cos[...] + pltpu.roll(block, HEAD_DIM // 2, 1) * turn_sin[...]

    def each(rows_of):
        return jnp.concatenate([rows_of(i) for i in range(lc)], axis=0)

    def rows_at(i):
        return slice(i * group, (i + 1) * group)

    def att_copy(t, h, peer, slot):
        return remote(
            att.at[t, h], att_in.at[t, h, slot], att_s.at[t], att_r.at[t, h], (sec, peer)
        )

    def all_att(t, h):
        return remote(
            att_in.at[t, h, pl.ds(1, n - 1)],
            att_in.at[t, h, pl.ds(1, n - 1)],
            att_s.at[t],
            att_r.at[t, h],
            (sec, me),
        )

    def summed(t, phase):
        with jax.named_scope("rs_wait"):
            remote(
                part.at[t, phase, pl.ds(1, n - 1)],
                part_in.at[t, phase, pl.ds(1, n - 1)],
                part_s.at[t],
                part_r.at[t, phase],
                (sec, me),
            ).wait_recv()
        result = part_in[t, phase, 0].astype(F32)
        for p in range(1, n):
            result = result + part_in[t, phase, p].astype(F32)
        return result

    def attention(t):
        with jax.named_scope("sq_wait"):
            remote(
                sq_in.at[t, pl.ds(1, n - 1)],
                sq_in.at[t, pl.ds(1, n - 1)],
                sq_s.at[t],
                sq_r.at[t],
                (sec, me),
            ).wait_recv()
        squares = sq_in[t, 0]
        for p in range(1, n):
            squares = squares + sq_in[t, p]
        factor = lax.rsqrt(
            jnp.sum(
                jnp.where(own_lane == own_request, squares, 0.0), axis=1, keepdims=True
            )
            / (n * width)
            + EPS
        )
        fresh_bias = bias_rows[t, HEADS:, :]
        block = summed(t, phases - 1) * factor + each(lambda i: fresh_bias)
        fresh[...] = jnp.where(is_key, turned(block), block).astype(BF16).astype(F32)
        if t == 1:
            kv_copy.wait()
        else:
            help_copies[3].wait_recv()

        def attend(h, carry):
            block_sum = summed(t, h)
            with jax.named_scope("attend"):
                bias_h = bias_rows[t, pl.ds(pl.multiple_of(h * group, group), group), :]
                query = turned(block_sum * factor + each(lambda i: bias_h))
                scores = each(
                    lambda i: lax.dot_general(
                        query[rows_at(i)].astype(BF16),
                        kv[t, i, 0, h],
                        (((1,), (1,)), ((), ())),
                        preferred_element_type=F32,
                    )
                )
                scores = scores * scale
                repeat = lambda row: jnp.broadcast_to(
                    fresh[pl.ds(row, 1), :], (group, HEAD_DIM)
                )
                key_new = each(lambda i: repeat(i * group + h))
                value_new = each(lambda i: repeat(i * group + KV_HEADS + h))
                self_score = (
                    jnp.sum(query.astype(BF16).astype(F32) * key_new, axis=1, keepdims=True)
                    * scale
                )
                visible = pos < own_rows[:, 0:1]
                top = jnp.maximum(
                    jnp.max(jnp.where(visible, scores, -1e30), axis=1, keepdims=True),
                    self_score,
                )
                weights = jnp.where(visible, jnp.exp(scores - top), 0.0)
                self_weight = jnp.exp(self_score - top)
                denominator = jnp.sum(weights, axis=1, keepdims=True) + self_weight
                mixed = each(
                    lambda i: jnp.dot(
                        weights[rows_at(i)].astype(BF16),
                        kv[t, i, 1, h],
                        preferred_element_type=F32,
                    )
                )
                mixed = mixed + self_weight.astype(BF16).astype(F32) * value_new
                att[t, h] = (mixed / denominator).astype(BF16)
            for peer in far_peers:
                att_copy(t, h, peer, me).start()
            att_in[t, h, me] = att[t, h]
            return carry

        lax.fori_loop(0, KV_HEADS, attend, 0)
        if t == 1:
            wo_copy.wait()
        else:
            help_copies[4].wait_recv()
        update[...] = x[...].astype(F32)

        def project_out(h, carry):
            mat = gathered(t, h)
            depth = pl.ds(pl.multiple_of(h * cw, cw), cw)
            update[...] += jnp.dot(mat, wo[t, depth, :], preferred_element_type=F32)
            return carry

        lax.fori_loop(0, KV_HEADS - 1, project_out, 0)

    def gathered(t, h):
        with jax.named_scope("ag_wait"):
            all_att(t, h).wait_recv()
        for p in range(n):
            stage[p * span : (p + 1) * span, :] = att_in[t, h, p].astype(F32)
        return jnp.concatenate(
            [stage[pl.ds(j, rows, stride=group), :].astype(BF16) for j in range(group)],
            axis=1,
        )

    top_rows = (KV_HEADS - 1) * cw

    def grown(t, mat, cols):
        return (
            update[:, cols]
            + jnp.dot(
                mat, wo[t, top_rows : top_rows + cw, cols], preferred_element_type=F32
            )
        ).astype(BF16)

    @pl.when(sec == 0)
    def _():
        sq_send(1)
        lax.fori_loop(0, early, send_only, 0)

    @pl.when(core == 1)
    def _():
        gain_copy.wait()
        with jax.named_scope("hop_wait"):
            remote(xo, x, hop_s, hop_r, (sec - 1, me)).wait_recv()

    @pl.when(helped)
    def _():
        help_copies[0].wait_recv()
        help_copies[1].wait_recv()
        help_copies[2].wait_recv()
        scale_rows(0)
        sq_send(0)
        lax.fori_loop(0, phases, project(0), 0)
        set_bias(0)
        attention(0)
        x[...] = grown(0, gathered(0, KV_HEADS - 1), slice(0, width))

    @pl.when(core == 1)
    def _():
        scale_rows(1)
        sq_send(1)

    @pl.when(runs)
    def _():
        lax.fori_loop(jnp.where(sec == 0, early, 0), phases, project(1), 0)

    @pl.when(sec == 0)
    def _():
        kv_copy.start()
        wo_copy.start()
        hw_copy.start()
        set_up()

    def fin_copy(c, peer, slot):
        return remote(
            fin.at[core, slot, c],
            fin.at[core, slot, c],
            fin_s,
            fin_r.at[slot],
            (sec, peer),
        )

    def sib_copy(c, piece, slot):
        return remote(
            fin.at[piece, slot, c],
            fin.at[piece, slot, c],
            sib_s,
            sib_r.at[slot],
            (sibling, me),
        )

    def fsq_copy(peer, slot):
        return remote(
            fsq_in.at[slot], fsq_in.at[slot], fsq_s, fsq_r, (sec, peer)
        )

    def fin_send():
        for k in (1, 6, 4, 5, 7, 2, 3) if relayed else range(1, n):
            if relayed and k in (5, 7):

                @pl.when(jnp.logical_not(outer))
                def _():
                    fin_copy(0, to_peer(k), me).start()

            else:
                fin_copy(0, to_peer(k), me).start()

    def side_copy(slot):
        return remote(
            fin.at[core, slot], fin.at[core, slot], side_s, fin_r.at[slot], (sec, to_peer(1))
        )

    def fp_copy(c, k):
        to = lax.rem(sec + k, sections)
        piece = lax.rem(to, 2)
        return remote(
            fin.at[piece, me, c], fin.at[piece, me, c], fp_s, fp_r.at[c], (to, me)
        )

    def fp_sq(k):
        to = lax.rem(sec + k, sections)
        return remote(
            fsq_in.at[me], fsq_in.at[me], fq_s, fp_r.at[chunks], (to, me)
        )

    @pl.when(runs)
    def _():
        attention(1)
        mat = gathered(1, KV_HEADS - 1)
        final_sq = jnp.zeros((rows, 1), F32)
        for c in range(parts):
            cols = slice(c * cut, (c + 1) * cut)
            new = grown(1, mat, cols)
            xo[:, cols] = new
            final = new.astype(F32)
            final_sq = final_sq + jnp.sum(final * final, axis=1, keepdims=True)

            @pl.when(sec < last)
            def _():
                hop_copy(c, following).start()

            @pl.when(sec == last)
            def _():
                lanes = cut // 128
                row = jnp.concatenate(
                    [
                        final_v[c * lanes + i : c * lanes + i + 1, :].astype(F32)
                        for i in range(lanes)
                    ],
                    axis=1,
                )
                both = (final * row).astype(BF16)
                fin[0, me, 0, :, cols] = both[:half]
                fin[1, me, 0, :, cols] = both[half:]

        @pl.when(sec == last)
        def _():
            for k in range(1, sections):
                fp_copy(0, k).start()
            fin_send()
            sib_copy(0, core, me).start()
            fsq_in[me] = to_row(final_sq)
            for k in range(1, sections):
                fp_sq(k).start()
            for peer in far_peers:
                fsq_copy(peer, me).start()

    @pl.when(sec < last)
    def _():
        for c in range(chunks):
            arriving = remote(
                fin.at[core, me, c], fin.at[core, me, c], fp_s, fp_r.at[c], (last, me)
            )
            with jax.named_scope("fp_wait"):
                arriving.wait_recv()
            fin_send()

            @pl.when(sec < last - 1)
            def _():
                sib_copy(c, core, me).start()

        arriving = remote(
            fsq_in.at[me], fsq_in.at[me], fq_s, fp_r.at[chunks], (last, me)
        )
        arriving.wait_recv()
        for peer in far_peers:
            fsq_copy(peer, me).start()

    hw_copy.wait()

    def whole(piece, slot, send, recv):
        return remote(fin.at[piece, slot], fin.at[piece, slot], send, recv.at[slot], (sibling, me))

    arrivals = [0, 1, far, 2, 3, 10 - far, 11 - far, far + 1]

    def arriving_from(k):
        return mate(me, arrivals[k] if relayed else k, n)[1]

    def pass_on(k):
        peer = arriving_from(k)
        with jax.named_scope("fin_wait"):
            whole(core, peer, fin_s, fin_r).wait_recv()
        if relayed and k == 2:
            side_copy(peer).start()

        for c in range(chunks):
            sib_copy(c, core, peer).start()

    def head(k, logits):
        peer = arriving_from(k)
        if isinstance(k, int) and k == 0:

            @pl.when(sec < last)
            def _():
                whole(1 - core, peer, sib_s, sib_r).wait_recv()

        else:
            with jax.named_scope("sib_wait"):
                whole(1 - core, peer, sib_s, sib_r).wait_recv()
        for c in range(chunks):
            at = pl.ds(pl.multiple_of(peer * width + c * chunk, chunk), chunk)
            both = jnp.concatenate([fin[0, peer, c], fin[1, peer, c]], axis=0)
            logits = logits + jnp.dot(both, hw[at, :], preferred_element_type=F32)
        return logits

    lag = min(2, n - 1)
    for k in range(1, lag + 1):
        pass_on(k)
    logits = head(0, jnp.zeros(out.shape, F32))

    def step(k, logits):
        pass_on(k)
        return head(k - lag, logits)

    if relayed:
        for k in range(lag + 1, n):
            logits = step(k, logits)
        for k in range(n - lag, n):
            logits = head(k, logits)
    else:
        logits = lax.fori_loop(lag + 1, n, step, logits)
        logits = lax.fori_loop(n - lag, n, head, logits)
    all_fsq = remote(
        fsq_in.at[pl.ds(1, n - 1)], fsq_in.at[pl.ds(1, n - 1)], fsq_s, fsq_r, (sec, me)
    )
    all_fsq.wait_recv()
    squares = jnp.sum(fsq_in[:, 0, :], axis=0, keepdims=True)
    logits = logits * lax.rsqrt(to_col(squares) / (n * width) + EPS)
    vocab = out.shape[1]
    ids = (mine * vocab + lax.broadcasted_iota(jnp.int32, (1, vocab), 1)).astype(F32)
    picked = jnp.sum(jnp.where(ids == target_v[:, 0:1], logits, 0.0), axis=1, keepdims=True)
    top = jnp.max(logits, axis=1, keepdims=True)
    amount = jnp.sum(jnp.exp(logits - top), axis=1, keepdims=True)
    row_of = lax.broadcasted_iota(jnp.int32, (rows, 128), 0)
    lane_of = lax.broadcasted_iota(jnp.int32, (rows, 128), 1)
    packed = jnp.where(lane_of == row_of, top, 0.0)
    packed = jnp.where(lane_of == row_of + rows, amount, packed)
    packed = jnp.where(lane_of == row_of + 2 * rows, picked, packed)
    red[...] = jnp.sum(packed, axis=0, keepdims=True)

    def red_copy(other, slot):
        return remote(
            red, red_in.at[slot], red_s, red_r, (other // n, lax.rem(other, n))
        )

    if total <= 64:
        for k in range(total - 1, 0, -1):
            red_copy(mate(mine, k, total)[0], mine).start()
    else:

        def red_start(k, carry):
            red_copy(mate(mine, total - k, total)[0], mine).start()
            return carry

        lax.fori_loop(1, total, red_start, 0)
    red_in[mine] = red[...]
    flat[...] = logits

    def sent(ref, sem):
        remote(ref, ref, sem, sem, (sec, me)).wait_send()

    others_n = pl.ds(1, n - 1)

    def stage_sent(t):
        sent(sq_in.at[t, others_n], sq_s.at[t])
        sent(part_in.at[t, :, others_n], part_s.at[t])
        sent(att_in.at[t, :, others_n], att_s.at[t])

    @pl.when(helped)
    def _():
        stage_sent(0)

    @pl.when(runs)
    def _():
        stage_sent(1)

    @pl.when(helps)
    def _():
        for copy in help_copies:
            copy.wait_send()

    if relayed:
        sent(fin.at[0, pl.ds(0, n - 3)], fin_s)
        sent(fin.at[0, 0], side_s)

        @pl.when(jnp.logical_not(outer))
        def _():
            sent(fin.at[0, pl.ds(0, 2)], fin_s)

    else:
        sent(fin.at[0, others_n], fin_s)
    sent(fin.at[0, others_n], sib_s)
    all_fsq.wait_send()

    @pl.when(sec != last - 1)
    def _():
        sent(fin.at[0, 0], sib_s)

    @pl.when((sec < last) & runs)
    def _():
        sent(xo, hop_s)

    @pl.when(sec == last)
    def _():
        sent(fin.at[0, pl.ds(1, sections - 1)], fp_s)
        sent(fsq_in.at[pl.ds(1, sections - 1)], fq_s)

    order = (
        jnp.sum(jnp.where(small_eye, slot_v[...].astype(F32), 0.0), axis=1, keepdims=True)
        == lane_of.astype(F32)
    )
    for s in range(rows):
        out[s : s + 1, :] = flat[pl.ds(slot_s[0, s], 1), :]

    everyone = remote(
        red_in.at[pl.ds(1, total - 1)],
        red_in.at[pl.ds(1, total - 1)],
        red_s,
        red_r,
        (sec, me),
    )
    with jax.named_scope("red_wait"):
        everyone.wait_recv()
    seen = red_in[:, 0, :]
    row_top = jnp.max(seen, axis=0, keepdims=True)
    amounts = pltpu.roll(seen, 128 - rows, 1)
    row_total = jnp.sum(amounts * jnp.exp(jnp.minimum(seen - row_top, 0.0)), axis=0, keepdims=True)
    log_total = row_top + jnp.log(row_total)
    total_col = jnp.sum(jnp.where(order, log_total, 0.0), axis=1, keepdims=True)
    out[...] = out[...] - total_col
    scored = pltpu.roll(jnp.sum(seen, axis=0, keepdims=True), 128 - 2 * rows, 1) - log_total
    chosen[...] = to_row(jnp.sum(jnp.where(order, scored, 0.0), axis=1, keepdims=True))
    with jax.named_scope("red_sent"):
        everyone.wait_send()


def local(
    hidden_in,
    lengths,
    assign,
    token_ids,
    attn_gain,
    qkv_weight,
    qkv_bias,
    out_weight,
    kv_cache,
    final_gain,
    head_weight,
):
    sections = lax.axis_size("pipe")
    n = lax.axis_size("mp")
    rows, width = hidden_in.shape
    lc = kv_cache.shape[1]
    qkv = qkv_weight.shape[2]
    inner = out_weight.shape[1]
    vocab = head_weight.shape[1]
    heads_all = HEADS + 2 * KV_HEADS
    half = HEAD_DIM // 2
    frequency = np.float32(THETA) ** (
        -np.arange(half).astype(np.float32) * np.float32(2.0) / np.float32(HEAD_DIM)
    )
    freq = jnp.asarray(np.concatenate([frequency, frequency])[None, :], F32)
    group = HEADS // KV_HEADS
    phases = heads_all // group
    span = lc * group
    dma = pltpu.SemaphoreType.DMA
    vm = pl.BlockSpec(memory_space=pltpu.VMEM)
    hbm = pl.BlockSpec(memory_space=pltpu.HBM)
    total = sections * n
    chunks = 1
    logprobs, chosen = pl.pallas_call(
        functools.partial(kernel, sections, n),
        out_shape=(
            pltpu.VMEM((rows, vocab), F32),
            pltpu.VMEM((1, 128), F32),
        ),
        in_specs=[hbm] * 12,
        out_specs=(vm, vm),
        scratch_shapes=[
            pltpu.VMEM((2, width, qkv), BF16),
            pltpu.VMEM((2, inner, width), BF16),
            pltpu.VMEM((2,) + kv_cache.shape[1:], BF16),
            pltpu.VMEM(head_weight.shape, BF16),
            pltpu.VMEM((rows, width), BF16),
            pltpu.VMEM((rows, width), BF16),
            pltpu.VMEM((rows, width), BF16),
            pltpu.VMEM((rows * group, HEAD_DIM), F32),
            pltpu.VMEM((2, phases, n, span, HEAD_DIM), BF16),
            pltpu.VMEM((2, phases, n, span, HEAD_DIM), BF16),
            pltpu.VMEM((2, 1, 128), F32),
            pltpu.VMEM((2, n, 1, 128), F32),
            pltpu.VMEM((2, 1, width), BF16),
            pltpu.VMEM((2, 1, qkv), BF16),
            pltpu.VMEM((width // 128, 128), BF16),
            pltpu.VMEM((1, rows), jnp.int32),
            pltpu.VMEM((1, rows), jnp.int32),
            pltpu.VMEM((1, rows), jnp.int32),
            pltpu.VMEM((1, HEAD_DIM), F32),
            pltpu.SMEM((1, rows), jnp.int32),
            pltpu.VMEM((2, heads_all, HEAD_DIM), F32),
            pltpu.VMEM((span, HEAD_DIM), F32),
            pltpu.VMEM((span, HEAD_DIM), F32),
            pltpu.VMEM((span, HEAD_DIM), F32),
            pltpu.VMEM((rows, 128), F32),
            pltpu.VMEM((span, HEAD_DIM), F32),
            pltpu.VMEM((2, KV_HEADS, span, HEAD_DIM), BF16),
            pltpu.VMEM((2, KV_HEADS, n, span, HEAD_DIM), BF16),
            pltpu.VMEM((rows, width), F32),
            pltpu.VMEM((2, n, chunks, rows // 2, width // chunks), BF16),
            pltpu.VMEM((n, 1, 128), F32),
            pltpu.VMEM((1, 128), F32),
            pltpu.VMEM((total, 1, 128), F32),
            pltpu.VMEM((rows, vocab), F32),
            dma((phases,)),
            dma((3,)),
            dma((9,)),
            dma((2,)),
            dma((2, phases)),
            dma((2,)),
            dma((2,)),
            dma((2,)),
            dma((2, KV_HEADS)),
            dma,
            dma,
            dma,
            dma((n,)),
            dma,
            dma((n,)),
            dma,
            dma,
            dma,
            dma,
            dma((chunks + 1,)),
            dma,
            dma,
            dma,
            dma((5,)),
            dma,
        ],
        compiler_params=pltpu.CompilerParams(
            collective_id=0, has_side_effects=True, vmem_limit_bytes=60 * 1024 * 1024
        ),
    )(
        hidden_in,
        lengths.reshape(1, rows),
        assign.reshape(1, rows),
        token_ids.reshape(1, rows),
        attn_gain,
        qkv_weight,
        qkv_bias,
        out_weight,
        kv_cache,
        final_gain.reshape(width // 128, 128),
        head_weight,
        freq,
    )
    return logprobs, chosen[0, :rows]


def solution(mesh):
    return jax.shard_map(
        local,
        mesh=mesh,
        in_specs=(
            P(None, "mp"),
            P(),
            P(),
            P(),
            P("pipe", "mp"),
            P("pipe", "mp", None),
            P("pipe", None),
            P("pipe", None, "mp"),
            P("pipe", "mp", None, None, None, None),
            P("mp"),
            P(None, ("pipe", "mp")),
        ),
        out_specs=(P(None, ("pipe", "mp")), P()),
        check_vma=False,
    )
```

```python
import functools

import jax
import jax.numpy as jnp
import numpy as np
from jax import lax
from jax.experimental import pallas as pl
from jax.experimental.pallas import tpu as pltpu
from jax.sharding import PartitionSpec as P

HEADS = 32
KV_HEADS = 4
HEAD_DIM = 128
EPS = 1e-06
THETA = 1000000.0
MESH = pl.DeviceIdType.MESH
F32 = jnp.float32
BF16 = jnp.bfloat16


def remote(src, dst, send_sem, recv_sem, device):
    return pltpu.make_async_remote_copy(
        src_ref=src,
        dst_ref=dst,
        send_sem=send_sem,
        recv_sem=recv_sem,
        device_id=device,
        device_id_type=MESH,
    )


def kernel(
    sections,
    n,
    hidden,
    lengths,
    assign,
    token_ids,
    gain,
    qkv_weight,
    bias,
    out_weight,
    cache,
    final_gain,
    head_weight,
    freq,
    out,
    chosen,
    wq,
    wo,
    kv,
    hw,
    x,
    xo,
    scaled,
    stage,
    part,
    part_in,
    sq,
    sq_in,
    gain_v,
    bias_v,
    final_v,
    len_v,
    slot_v,
    token_v,
    freq_v,
    slot_s,
    bias_rows,
    turn_cos,
    turn_sin,
    own_rows,
    target_v,
    fresh,
    att,
    att_in,
    update,
    fin,
    fsq_in,
    red,
    red_in,
    flat,
    wq_sem,
    w_sem,
    small_sem,
    part_s,
    part_r,
    sq_s,
    sq_r,
    att_s,
    att_r,
    hop_s,
    hop_r,
    fin_s,
    fin_r,
    sib_s,
    sib_r,
    fsq_s,
    fsq_r,
    fp_s,
    fq_s,
    fp_r,
    red_s,
    red_r,
    help_s,
    help_r,
    side_s,
):
    sec = lax.axis_index("pipe")
    me = lax.axis_index("mp")
    total = sections * n
    rows, width = x.shape
    lc = kv.shape[1]
    heads_all = HEADS + 2 * KV_HEADS
    group = HEADS // KV_HEADS
    phases = heads_all // group
    span = lc * group
    last = sections - 1
    scale = HEAD_DIM ** (-0.5)
    cw = group * HEAD_DIM
    half = rows // 2
    chunks = fin.shape[2]
    chunk = width // chunks
    parts = 1
    cut = width // parts
    core = lax.rem(sec, 2)
    sibling = sec + 1 - 2 * core
    mine = sec * n + me
    runs = (sec < 2) | (core == 1)
    helps = (sec >= 2) & (core == 0)
    helped = (sec >= 2) & (core == 1)
    following = jnp.where(sec == 0, 1, sec + 2)
    early = min(1, phases)

    def mate(own, k, count):
        if count & (count - 1):
            return lax.rem(own + k, count), lax.rem(own + count - k, count)
        other = 0
        for b in range(count.bit_length() - 1):
            place = 1 << b
            mine_bit = lax.rem(own // place, 2)
            if isinstance(k, int):
                bit = 1 - mine_bit if (k // place) % 2 else mine_bit
            else:
                flip = lax.rem(k // place, 2)
                bit = mine_bit + flip - 2 * mine_bit * flip
            other = other + place * bit
        return other, other

    pairs = [mate(me, k, n) for k in range(n)]
    across = max(d for d in range(1, n + 1) if n % d == 0 and d * d <= n)
    relayed = across == 2 and n == 8
    place = me // across
    outer = (place == 0) | (place == n // across - 1)
    far = jnp.where(outer, 6, 4)
    if relayed:
        far_peers = [
            mate(me, k, n)[0] for k in (far + 1, far, 11 - far, 10 - far, 3, 2, 1)
        ]
    else:
        far_peers = [pairs[k][0] for k in range(n - 1, 0, -1)]

    def to_peer(k):
        return pairs[k][0]

    def from_peer(k):
        return pairs[k][1]

    def wq_copy(c):
        cols = pl.ds(pl.multiple_of(c * cw, cw), cw)
        return pltpu.make_async_copy(qkv_weight.at[0, :, cols], wq.at[1, :, cols], wq_sem.at[c])

    def phase_of(k):
        return lax.rem(k + phases - 1, phases)

    def small(i, src, dst):
        return pltpu.make_async_copy(src, dst, small_sem.at[i])

    hidden_copy = small(0, hidden, x)
    gain_copy = small(1, gain, gain_v.at[1])
    others = [
        small(2, bias, bias_v.at[1]),
        small(3, final_gain, final_v),
        small(4, lengths, len_v),
        small(5, assign, slot_v),
        small(6, token_ids, token_v),
        small(7, freq, freq_v),
        small(8, assign, slot_s),
    ]

    @pl.when(sec == 0)
    def _():
        hidden_copy.start()

    @pl.when(runs)
    def _():
        gain_copy.start()
        for k in range(early):
            wq_copy((k + phases - 1) % phases).start()

    def wq_rest():
        for k in range(early, phases):
            wq_copy((k + phases - 1) % phases).start()

    kv_copy = pltpu.make_async_copy(cache.at[0], kv.at[1], w_sem.at[0])
    wo_copy = pltpu.make_async_copy(out_weight.at[0], wo.at[1], w_sem.at[1])
    hw_copy = pltpu.make_async_copy(head_weight, hw, w_sem.at[2])

    barrier = pltpu.get_barrier_semaphore()
    for peer in far_peers:
        pl.semaphore_signal(barrier, inc=1, device_id=(sec, peer), device_id_type=MESH)
    for k in range(1, sections):
        pl.semaphore_signal(
            barrier, inc=1, device_id=(lax.rem(sec + k, sections), me), device_id_type=MESH
        )
    @pl.when(sec > 0)
    def _():
        for copy in others:
            copy.start()
        hw_copy.start()

    @pl.when((sec > 0) & runs)
    def _():
        wq_rest()
        kv_copy.start()
        wo_copy.start()

    def help_copy(i, src, dst):
        return remote(src, dst, help_s, help_r.at[i], (sibling, me))

    help_copies = [
        help_copy(0, gain, gain_v.at[0]),
        help_copy(1, bias, bias_v.at[0]),
        help_copy(2, qkv_weight.at[0], wq.at[0]),
        help_copy(3, cache.at[0], kv.at[0]),
        help_copy(4, out_weight.at[0], wo.at[0]),
    ]

    eye = lax.broadcasted_iota(jnp.int32, (rows, 128), 0) == lax.broadcasted_iota(
        jnp.int32, (rows, 128), 1
    )

    def to_row(col):
        return jnp.sum(jnp.where(eye, col, 0.0), axis=0, keepdims=True)

    def to_col(row):
        return jnp.sum(jnp.where(eye, row, 0.0), axis=1, keepdims=True)

    lane = lax.broadcasted_iota(jnp.int32, (1, HEAD_DIM), 1)
    lane_rows = lax.broadcasted_iota(jnp.int32, (1, rows), 1)
    small_eye = lax.broadcasted_iota(jnp.int32, (rows, rows), 0) == lax.broadcasted_iota(
        jnp.int32, (rows, rows), 1
    )

    def set_bias(t):
        for i in range(heads_all):
            bias_rows[t, i : i + 1, :] = bias_v[
                t, :, i * HEAD_DIM : (i + 1) * HEAD_DIM
            ].astype(F32)

    def set_up():
        for copy in others:
            copy.wait()
        set_bias(1)
        target = jnp.sum(
            jnp.where(small_eye, token_v[...].astype(F32), 0.0), axis=1, keepdims=True
        )
        target_v[...] = jnp.broadcast_to(target, target_v.shape)
        length = jnp.concatenate(
            [
                jnp.sum(
                    jnp.where(lane_rows == me * lc + i, len_v[...].astype(F32), 0.0),
                    axis=1,
                    keepdims=True,
                )
                for i in range(lc)
            ],
            axis=0,
        )
        angles = length * freq_v[...]
        cosines = jnp.cos(angles)
        sines = jnp.sin(angles) * jnp.where(lane < HEAD_DIM // 2, -1.0, 1.0)
        for i in range(lc):
            own = slice(i * group, (i + 1) * group)
            own_rows[own, :] = jnp.broadcast_to(length[i : i + 1], (group, HEAD_DIM))
            turn_cos[own, :] = jnp.broadcast_to(cosines[i : i + 1], (group, HEAD_DIM))
            turn_sin[own, :] = jnp.broadcast_to(sines[i : i + 1], (group, HEAD_DIM))

    def scale_rows(t):
        current = x[...].astype(F32)
        sq[t] = to_row(jnp.sum(current * current, axis=1, keepdims=True))
        scaled[...] = (current * gain_v[t].astype(F32)).astype(BF16)

    def sq_copy(t, peer, slot):
        return remote(sq.at[t], sq_in.at[t, slot], sq_s.at[t], sq_r.at[t], (sec, peer))

    def sq_send(t):
        for peer in far_peers:
            sq_copy(t, peer, me).start()
        sq_in[t, me] = sq[t]

    def part_copy(t, phase, peer, slot):
        return remote(
            part.at[t, phase, peer],
            part_in.at[t, phase, slot],
            part_s.at[t],
            part_r.at[t, phase],
            (sec, peer),
        )

    def multiply(t, phase):
        if t == 1:
            wq_copy(phase).wait()
        base = pl.multiple_of(phase * cw, cw)
        piece = jnp.dot(scaled[...], wq[t, :, pl.ds(base, cw)], preferred_element_type=F32)
        for j in range(group):
            stage[pl.ds(j, rows, stride=group), :] = piece[
                :, j * HEAD_DIM : (j + 1) * HEAD_DIM
            ]
        for p in range(n):
            part[t, phase, p] = stage[p * span : (p + 1) * span, :].astype(BF16)

    def spread(t, phase):
        for peer in far_peers:
            part_copy(t, phase, peer, me).start()
        part_in[t, phase, me] = part[t, phase, me]

    def compute_only(k, carry):
        multiply(1, phase_of(k))
        return carry

    def send_only(k, carry):
        spread(1, phase_of(k))
        return carry

    def project(t):
        def one(k, carry):
            multiply(t, phase_of(k))
            spread(t, phase_of(k))
            return carry

        return one

    def hop_copy(c, to):
        cols = pl.ds(c * cut, cut)
        return remote(xo.at[:, cols], x.at[:, cols], hop_s, hop_r, (to, me))


    @pl.when(sec == 0)
    def _():
        with jax.named_scope("hidden_wait"):
            hidden_copy.wait()
        gain_copy.wait()
        scale_rows(1)
        wq_rest()
        for copy in others:
            copy.start()
        lax.fori_loop(0, early, compute_only, 0)

    @pl.when(sec > 0)
    def _():
        set_up()

    with jax.named_scope("barrier"):
        pl.semaphore_wait(barrier, n + sections - 2)

    @pl.when(helps)
    def _():
        for copy in help_copies:
            copy.start()

    pos = lax.broadcasted_iota(jnp.int32, (1, kv.shape[4]), 1).astype(F32)
    own_request = me * lc + lax.broadcasted_iota(jnp.int32, (span, 128), 0) // group
    own_lane = lax.broadcasted_iota(jnp.int32, (span, 128), 1)
    is_key = (
        lax.rem(lax.broadcasted_iota(jnp.int32, (span, HEAD_DIM), 0), 2 * KV_HEADS) < KV_HEADS
    )

    def turned(block):
        return block * turn_cos[...] + pltpu.roll(block, HEAD_DIM // 2, 1) * turn_sin[...]

    def each(rows_of):
        return jnp.concatenate([rows_of(i) for i in range(lc)], axis=0)

    def rows_at(i):
        return slice(i * group, (i + 1) * group)

    def att_copy(t, h, peer, slot):
        return remote(
            att.at[t, h], att_in.at[t, h, slot], att_s.at[t], att_r.at[t, h], (sec, peer)
        )

    def all_att(t, h):
        return remote(
            att_in.at[t, h, pl.ds(1, n - 1)],
            att_in.at[t, h, pl.ds(1, n - 1)],
            att_s.at[t],
            att_r.at[t, h],
            (sec, me),
        )

    def summed(t, phase):
        with jax.named_scope("rs_wait"):
            remote(
                part.at[t, phase, pl.ds(1, n - 1)],
                part_in.at[t, phase, pl.ds(1, n - 1)],
                part_s.at[t],
                part_r.at[t, phase],
                (sec, me),
            ).wait_recv()
        result = part_in[t, phase, 0].astype(F32)
        for p in range(1, n):
            result = result + part_in[t, phase, p].astype(F32)
        return result

    def attention(t):
        with jax.named_scope("sq_wait"):
            remote(
                sq_in.at[t, pl.ds(1, n - 1)],
                sq_in.at[t, pl.ds(1, n - 1)],
                sq_s.at[t],
                sq_r.at[t],
                (sec, me),
            ).wait_recv()
        squares = sq_in[t, 0]
        for p in range(1, n):
            squares = squares + sq_in[t, p]
        factor = lax.rsqrt(
            jnp.sum(
                jnp.where(own_lane == own_request, squares, 0.0), axis=1, keepdims=True
            )
            / (n * width)
            + EPS
        )
        fresh_bias = bias_rows[t, HEADS:, :]
        block = summed(t, phases - 1) * factor + each(lambda i: fresh_bias)
        fresh[...] = jnp.where(is_key, turned(block), block).astype(BF16).astype(F32)
        if t == 1:
            kv_copy.wait()
        else:
            help_copies[3].wait_recv()

        def attend(h, carry):
            block_sum = summed(t, h)
            with jax.named_scope("attend"):
                bias_h = bias_rows[t, pl.ds(pl.multiple_of(h * group, group), group), :]
                query = turned(block_sum * factor + each(lambda i: bias_h))
                scores = each(
                    lambda i: lax.dot_general(
                        query[rows_at(i)].astype(BF16),
                        kv[t, i, 0, h],
                        (((1,), (1,)), ((), ())),
                        preferred_element_type=F32,
                    )
                )
                scores = scores * scale
                repeat = lambda row: jnp.broadcast_to(
                    fresh[pl.ds(row, 1), :], (group, HEAD_DIM)
                )
                key_new = each(lambda i: repeat(i * group + h))
                value_new = each(lambda i: repeat(i * group + KV_HEADS + h))
                self_score = (
                    jnp.sum(query.astype(BF16).astype(F32) * key_new, axis=1, keepdims=True)
                    * scale
                )
                visible = pos < own_rows[:, 0:1]
                top = jnp.maximum(
                    jnp.max(jnp.where(visible, scores, -1e30), axis=1, keepdims=True),
                    self_score,
                )
                weights = jnp.where(visible, jnp.exp(scores - top), 0.0)
                self_weight = jnp.exp(self_score - top)
                denominator = jnp.sum(weights, axis=1, keepdims=True) + self_weight
                mixed = each(
                    lambda i: jnp.dot(
                        weights[rows_at(i)].astype(BF16),
                        kv[t, i, 1, h],
                        preferred_element_type=F32,
                    )
                )
                mixed = mixed + self_weight.astype(BF16).astype(F32) * value_new
                att[t, h] = (mixed / denominator).astype(BF16)
            for peer in far_peers:
                att_copy(t, h, peer, me).start()
            att_in[t, h, me] = att[t, h]
            return carry

        lax.fori_loop(0, KV_HEADS, attend, 0)
        if t == 1:
            wo_copy.wait()
        else:
            help_copies[4].wait_recv()
        update[...] = x[...].astype(F32)

        def project_out(h, carry):
            mat = gathered(t, h)
            depth = pl.ds(pl.multiple_of(h * cw, cw), cw)
            update[...] += jnp.dot(mat, wo[t, depth, :], preferred_element_type=F32)
            return carry

        lax.fori_loop(0, KV_HEADS - 1, project_out, 0)

    def gathered(t, h):
        with jax.named_scope("ag_wait"):
            all_att(t, h).wait_recv()
        for p in range(n):
            stage[p * span : (p + 1) * span, :] = att_in[t, h, p].astype(F32)
        return jnp.concatenate(
            [stage[pl.ds(j, rows, stride=group), :].astype(BF16) for j in range(group)],
            axis=1,
        )

    top_rows = (KV_HEADS - 1) * cw

    def grown(t, mat, cols):
        return (
            update[:, cols]
            + jnp.dot(
                mat, wo[t, top_rows : top_rows + cw, cols], preferred_element_type=F32
            )
        ).astype(BF16)

    @pl.when(sec == 0)
    def _():
        sq_send(1)
        lax.fori_loop(0, early, send_only, 0)

    @pl.when(core == 1)
    def _():
        gain_copy.wait()
        with jax.named_scope("hop_wait"):
            remote(xo, x, hop_s, hop_r, (sec - 1, me)).wait_recv()

    @pl.when(helped)
    def _():
        help_copies[0].wait_recv()
        help_copies[1].wait_recv()
        help_copies[2].wait_recv()
        scale_rows(0)
        sq_send(0)
        lax.fori_loop(0, phases, project(0), 0)
        set_bias(0)
        attention(0)
        x[...] = grown(0, gathered(0, KV_HEADS - 1), slice(0, width))

    @pl.when(core == 1)
    def _():
        scale_rows(1)
        sq_send(1)

    @pl.when(runs)
    def _():
        lax.fori_loop(jnp.where(sec == 0, early, 0), phases, project(1), 0)

    @pl.when(sec == 0)
    def _():
        kv_copy.start()
        wo_copy.start()
        hw_copy.start()
        set_up()

    def fin_copy(c, peer, slot):
        return remote(
            fin.at[core, slot, c],
            fin.at[core, slot, c],
            fin_s,
            fin_r.at[slot],
            (sec, peer),
        )

    def sib_copy(c, piece, slot):
        return remote(
            fin.at[piece, slot, c],
            fin.at[piece, slot, c],
            sib_s,
            sib_r.at[slot],
            (sibling, me),
        )

    def fsq_copy(peer, slot):
        return remote(
            fsq_in.at[slot], fsq_in.at[slot], fsq_s, fsq_r, (sec, peer)
        )

    def fin_send():
        for k in (1, 6, 4, 5, 7, 2, 3) if relayed else range(1, n):
            if relayed and k in (5, 7):

                @pl.when(jnp.logical_not(outer))
                def _():
                    fin_copy(0, to_peer(k), me).start()

            else:
                fin_copy(0, to_peer(k), me).start()

    def side_copy(slot):
        return remote(
            fin.at[core, slot], fin.at[core, slot], side_s, fin_r.at[slot], (sec, to_peer(1))
        )

    def fp_copy(c, k):
        to = lax.rem(sec + k, sections)
        piece = lax.rem(to, 2)
        return remote(
            fin.at[piece, me, c], fin.at[piece, me, c], fp_s, fp_r.at[c], (to, me)
        )

    def fp_sq(k):
        to = lax.rem(sec + k, sections)
        return remote(
            fsq_in.at[me], fsq_in.at[me], fq_s, fp_r.at[chunks], (to, me)
        )

    @pl.when(runs)
    def _():
        attention(1)
        mat = gathered(1, KV_HEADS - 1)
        final_sq = jnp.zeros((rows, 1), F32)
        for c in range(parts):
            cols = slice(c * cut, (c + 1) * cut)
            new = grown(1, mat, cols)
            xo[:, cols] = new
            final = new.astype(F32)
            final_sq = final_sq + jnp.sum(final * final, axis=1, keepdims=True)

            @pl.when(sec < last)
            def _():
                hop_copy(c, following).start()

            @pl.when(sec == last)
            def _():
                lanes = cut // 128
                row = jnp.concatenate(
                    [
                        final_v[c * lanes + i : c * lanes + i + 1, :].astype(F32)
                        for i in range(lanes)
                    ],
                    axis=1,
                )
                both = (final * row).astype(BF16)
                fin[0, me, 0, :, cols] = both[:half]
                fin[1, me, 0, :, cols] = both[half:]

        @pl.when(sec == last)
        def _():
            for k in range(1, sections):
                fp_copy(0, k).start()
            fin_send()
            sib_copy(0, core, me).start()
            fsq_in[me] = to_row(final_sq)
            for k in range(1, sections):
                fp_sq(k).start()
            for peer in far_peers:
                fsq_copy(peer, me).start()

    @pl.when(sec < last)
    def _():
        for c in range(chunks):
            arriving = remote(
                fin.at[core, me, c], fin.at[core, me, c], fp_s, fp_r.at[c], (last, me)
            )
            with jax.named_scope("fp_wait"):
                arriving.wait_recv()
            fin_send()

            @pl.when(sec < last - 1)
            def _():
                sib_copy(c, core, me).start()

        arriving = remote(
            fsq_in.at[me], fsq_in.at[me], fq_s, fp_r.at[chunks], (last, me)
        )
        arriving.wait_recv()
        for peer in far_peers:
            fsq_copy(peer, me).start()

    hw_copy.wait()

    def whole(piece, slot, send, recv):
        return remote(fin.at[piece, slot], fin.at[piece, slot], send, recv.at[slot], (sibling, me))

    arrivals = [0, 1, far, 2, 3, 10 - far, 11 - far, far + 1]

    def arriving_from(k):
        return mate(me, arrivals[k] if relayed else k, n)[1]

    def pass_on(k):
        peer = arriving_from(k)
        with jax.named_scope("fin_wait"):
            whole(core, peer, fin_s, fin_r).wait_recv()
        if relayed and k == 2:
            side_copy(peer).start()

        for c in range(chunks):
            sib_copy(c, core, peer).start()

    def head(k, logits):
        peer = arriving_from(k)
        if isinstance(k, int) and k == 0:

            @pl.when(sec < last)
            def _():
                whole(1 - core, peer, sib_s, sib_r).wait_recv()

        else:
            with jax.named_scope("sib_wait"):
                whole(1 - core, peer, sib_s, sib_r).wait_recv()
        for c in range(chunks):
            at = pl.ds(pl.multiple_of(peer * width + c * chunk, chunk), chunk)
            both = jnp.concatenate([fin[0, peer, c], fin[1, peer, c]], axis=0)
            logits = logits + jnp.dot(both, hw[at, :], preferred_element_type=F32)
        return logits

    lag = min(2, n - 1)
    for k in range(1, lag + 1):
        pass_on(k)
    logits = head(0, jnp.zeros(out.shape, F32))

    def step(k, logits):
        pass_on(k)
        return head(k - lag, logits)

    if relayed:
        for k in range(lag + 1, n):
            logits = step(k, logits)
        for k in range(n - lag, n):
            logits = head(k, logits)
    else:
        logits = lax.fori_loop(lag + 1, n, step, logits)
        logits = lax.fori_loop(n - lag, n, head, logits)
    all_fsq = remote(
        fsq_in.at[pl.ds(1, n - 1)], fsq_in.at[pl.ds(1, n - 1)], fsq_s, fsq_r, (sec, me)
    )
    all_fsq.wait_recv()
    squares = jnp.sum(fsq_in[:, 0, :], axis=0, keepdims=True)
    logits = logits * lax.rsqrt(to_col(squares) / (n * width) + EPS)
    vocab = out.shape[1]
    ids = (mine * vocab + lax.broadcasted_iota(jnp.int32, (1, vocab), 1)).astype(F32)
    picked = jnp.sum(jnp.where(ids == target_v[:, 0:1], logits, 0.0), axis=1, keepdims=True)
    top = jnp.max(logits, axis=1, keepdims=True)
    amount = jnp.sum(jnp.exp(logits - top), axis=1, keepdims=True)
    row_of = lax.broadcasted_iota(jnp.int32, (rows, 128), 0)
    lane_of = lax.broadcasted_iota(jnp.int32, (rows, 128), 1)
    packed = jnp.where(lane_of == row_of, top, 0.0)
    packed = jnp.where(lane_of == row_of + rows, amount, packed)
    packed = jnp.where(lane_of == row_of + 2 * rows, picked, packed)
    red[...] = jnp.sum(packed, axis=0, keepdims=True)

    def red_copy(other, slot):
        return remote(
            red, red_in.at[slot], red_s, red_r, (other // n, lax.rem(other, n))
        )

    if total <= 64:
        for k in range(total - 1, 0, -1):
            red_copy(mate(mine, k, total)[0], mine).start()
    else:

        def red_start(k, carry):
            red_copy(mate(mine, total - k, total)[0], mine).start()
            return carry

        lax.fori_loop(1, total, red_start, 0)
    red_in[mine] = red[...]
    flat[...] = logits

    def sent(ref, sem):
        remote(ref, ref, sem, sem, (sec, me)).wait_send()

    others_n = pl.ds(1, n - 1)

    def stage_sent(t):
        sent(sq_in.at[t, others_n], sq_s.at[t])
        sent(part_in.at[t, :, others_n], part_s.at[t])
        sent(att_in.at[t, :, others_n], att_s.at[t])

    @pl.when(helped)
    def _():
        stage_sent(0)

    @pl.when(runs)
    def _():
        stage_sent(1)

    @pl.when(helps)
    def _():
        for copy in help_copies:
            copy.wait_send()

    if relayed:
        sent(fin.at[0, pl.ds(0, n - 3)], fin_s)
        sent(fin.at[0, 0], side_s)

        @pl.when(jnp.logical_not(outer))
        def _():
            sent(fin.at[0, pl.ds(0, 2)], fin_s)

    else:
        sent(fin.at[0, others_n], fin_s)
    sent(fin.at[0, others_n], sib_s)
    all_fsq.wait_send()

    @pl.when(sec != last - 1)
    def _():
        sent(fin.at[0, 0], sib_s)

    @pl.when((sec < last) & runs)
    def _():
        sent(xo, hop_s)

    @pl.when(sec == last)
    def _():
        sent(fin.at[0, pl.ds(1, sections - 1)], fp_s)
        sent(fsq_in.at[pl.ds(1, sections - 1)], fq_s)

    order = (
        jnp.sum(jnp.where(small_eye, slot_v[...].astype(F32), 0.0), axis=1, keepdims=True)
        == lane_of.astype(F32)
    )
    for s in range(rows):
        out[s : s + 1, :] = flat[pl.ds(slot_s[0, s], 1), :]

    everyone = remote(
        red_in.at[pl.ds(1, total - 1)],
        red_in.at[pl.ds(1, total - 1)],
        red_s,
        red_r,
        (sec, me),
    )
    with jax.named_scope("red_wait"):
        everyone.wait_recv()
    seen = red_in[:, 0, :]
    row_top = jnp.max(seen, axis=0, keepdims=True)
    amounts = pltpu.roll(seen, 128 - rows, 1)
    row_total = jnp.sum(amounts * jnp.exp(jnp.minimum(seen - row_top, 0.0)), axis=0, keepdims=True)
    log_total = row_top + jnp.log(row_total)
    total_col = jnp.sum(jnp.where(order, log_total, 0.0), axis=1, keepdims=True)
    out[...] = out[...] - total_col
    scored = pltpu.roll(jnp.sum(seen, axis=0, keepdims=True), 128 - 2 * rows, 1) - log_total
    chosen[...] = to_row(jnp.sum(jnp.where(order, scored, 0.0), axis=1, keepdims=True))
    with jax.named_scope("red_sent"):
        everyone.wait_send()


def local(
    hidden_in,
    lengths,
    assign,
    token_ids,
    attn_gain,
    qkv_weight,
    qkv_bias,
    out_weight,
    kv_cache,
    final_gain,
    head_weight,
):
    sections = lax.axis_size("pipe")
    n = lax.axis_size("mp")
    rows, width = hidden_in.shape
    lc = kv_cache.shape[1]
    qkv = qkv_weight.shape[2]
    inner = out_weight.shape[1]
    vocab = head_weight.shape[1]
    heads_all = HEADS + 2 * KV_HEADS
    half = HEAD_DIM // 2
    frequency = np.float32(THETA) ** (
        -np.arange(half).astype(np.float32) * np.float32(2.0) / np.float32(HEAD_DIM)
    )
    freq = jnp.asarray(np.concatenate([frequency, frequency])[None, :], F32)
    group = HEADS // KV_HEADS
    phases = heads_all // group
    span = lc * group
    dma = pltpu.SemaphoreType.DMA
    vm = pl.BlockSpec(memory_space=pltpu.VMEM)
    hbm = pl.BlockSpec(memory_space=pltpu.HBM)
    total = sections * n
    chunks = 1
    logprobs, chosen = pl.pallas_call(
        functools.partial(kernel, sections, n),
        out_shape=(
            pltpu.VMEM((rows, vocab), F32),
            pltpu.VMEM((1, 128), F32),
        ),
        in_specs=[hbm] * 12,
        out_specs=(vm, vm),
        scratch_shapes=[
            pltpu.VMEM((2, width, qkv), BF16),
            pltpu.VMEM((2, inner, width), BF16),
            pltpu.VMEM((2,) + kv_cache.shape[1:], BF16),
            pltpu.VMEM(head_weight.shape, BF16),
            pltpu.VMEM((rows, width), BF16),
            pltpu.VMEM((rows, width), BF16),
            pltpu.VMEM((rows, width), BF16),
            pltpu.VMEM((rows * group, HEAD_DIM), F32),
            pltpu.VMEM((2, phases, n, span, HEAD_DIM), BF16),
            pltpu.VMEM((2, phases, n, span, HEAD_DIM), BF16),
            pltpu.VMEM((2, 1, 128), F32),
            pltpu.VMEM((2, n, 1, 128), F32),
            pltpu.VMEM((2, 1, width), BF16),
            pltpu.VMEM((2, 1, qkv), BF16),
            pltpu.VMEM((width // 128, 128), BF16),
            pltpu.VMEM((1, rows), jnp.int32),
            pltpu.VMEM((1, rows), jnp.int32),
            pltpu.VMEM((1, rows), jnp.int32),
            pltpu.VMEM((1, HEAD_DIM), F32),
            pltpu.SMEM((1, rows), jnp.int32),
            pltpu.VMEM((2, heads_all, HEAD_DIM), F32),
            pltpu.VMEM((span, HEAD_DIM), F32),
            pltpu.VMEM((span, HEAD_DIM), F32),
            pltpu.VMEM((span, HEAD_DIM), F32),
            pltpu.VMEM((rows, 128), F32),
            pltpu.VMEM((span, HEAD_DIM), F32),
            pltpu.VMEM((2, KV_HEADS, span, HEAD_DIM), BF16),
            pltpu.VMEM((2, KV_HEADS, n, span, HEAD_DIM), BF16),
            pltpu.VMEM((rows, width), F32),
            pltpu.VMEM((2, n, chunks, rows // 2, width // chunks), BF16),
            pltpu.VMEM((n, 1, 128), F32),
            pltpu.VMEM((1, 128), F32),
            pltpu.VMEM((total, 1, 128), F32),
            pltpu.VMEM((rows, vocab), F32),
            dma((phases,)),
            dma((3,)),
            dma((9,)),
            dma((2,)),
            dma((2, phases)),
            dma((2,)),
            dma((2,)),
            dma((2,)),
            dma((2, KV_HEADS)),
            dma,
            dma,
            dma,
            dma((n,)),
            dma,
            dma((n,)),
            dma,
            dma,
            dma,
            dma,
            dma((chunks + 1,)),
            dma,
            dma,
            dma,
            dma((5,)),
            dma,
        ],
        compiler_params=pltpu.CompilerParams(
            collective_id=0, has_side_effects=True, vmem_limit_bytes=60 * 1024 * 1024
        ),
    )(
        hidden_in,
        lengths.reshape(1, rows),
        assign.reshape(1, rows),
        token_ids.reshape(1, rows),
        attn_gain,
        qkv_weight,
        qkv_bias,
        out_weight,
        kv_cache,
        final_gain.reshape(width // 128, 128),
        head_weight,
        freq,
    )
    return logprobs, chosen[0, :rows]


def solution(mesh):
    return jax.shard_map(
        local,
        mesh=mesh,
        in_specs=(
            P(None, "mp"),
            P(),
            P(),
            P(),
            P("pipe", "mp"),
            P("pipe", "mp", None),
            P("pipe", None),
            P("pipe", None, "mp"),
            P("pipe", "mp", None, None, None, None),
            P("mp"),
            P(None, ("pipe", "mp")),
        ),
        out_specs=(P(None, ("pipe", "mp")), P()),
        check_vma=False,
    )
```
